256 devices in a mesh: sub: 64 (over y, z, x_lo), iter: 4 (over x_hi, core).
Axes of the slice: x: 4 (x_hi: 2, x_lo: 2; x = x_hi * 2 + x_lo), y: 4, z: 8, core: 2. Of those that a mesh axis runs over, the one named last changes fastest.
Arguments:
- fields: float32 [4, 128, 128, 128], P('iter', 'sub'), may hold values from -6 to 6
- labels: int32 [128, 128, 128], P('sub'), may hold values from 0 to 3
- traces: float32 [4, 64, 4, 128, 128], P('iter', 'sub'), may hold values from -6 to 6
- new_guess: float32 [2, 64, 4, 128, 128], P(None, 'sub'), may hold values from -6 to 6
- cond_table: float32 [4], replicated, may hold values from 0.2 to 5
- cap_table: float32 [4], replicated, may hold values from 0.5 to 4
Outputs:
- end_fields: float32 [4, 128, 128, 128], P('iter', 'sub')
- corrected: float32 [4, 64, 4, 128, 128], P('iter', 'sub')
The draws below stay inside these ranges and needn't reach their ends.
All inputs are finite; a program needn't handle non-finite values.
Results may differ from the reference program's by a relative error of at most 0.00002.
Values sent between devices are 32-bit elements; how exact they have to be, the bound alone decides.
A program may use at most 64 MiB of HBM per device.

```python
import math
import jax
import jax.numpy as jnp

CX = 2
NY = 128
NZ = 128
STEPS = 4
SWEEPS = 3
TICKS = 3
CLASSES = 4
GROUPS = 4
NX = 128
N_SUB = 64


def set_ends(entries, rng, low, largest):
    longest = entries.shape.index(max(entries.shape))
    spots = []
    for shift in (0, 1):
        where = [jax.random.randint(jax.random.fold_in(rng, axis), (), 0, length) for axis, length in enumerate(entries.shape)]
        where[longest] = (where[longest] + shift) % entries.shape[longest]
        spots.append(tuple(where))
    return entries.at[spots[0]].set(low).at[spots[1]].set(largest)


def block_scale(own_key, extent, split, smallest, top_value):
    def one(position, parts):
        draws = jax.random.uniform(jax.random.fold_in(jax.random.fold_in(own_key, 6), position), (parts,), jnp.float32, smallest / len(split), top_value / len(split))
        return jnp.repeat(jnp.exp(draws), extent[position] // parts).reshape((-1,) + (1,) * (len(extent) - position - 1))

    factor_of = one(*split[0])
    for cut in split[1:]:
        factor_of = factor_of * one(*cut)
    return factor_of


def scatter_about(rng, shape, width, limit, pieces=(), kind=jnp.bfloat16):
    values = width * jax.random.normal(rng, shape, jnp.float32)
    if pieces:
        values = values * block_scale(rng, shape, pieces, -0.22, 0.18)
    return jnp.clip(values, -limit, limit).astype(kind)


def setup_inputs(seed: int = 0) -> dict:
    seeds = jax.random.split(jax.random.key(seed), 7)
    fields = scatter_about(seeds[0], (GROUPS, NX, NY, NZ), 1.0, 6.0, ((0, 4), (1, 64)), jnp.float32)
    labels = set_ends(jax.random.randint(seeds[1], (NX, NY, NZ), 0, CLASSES), jax.random.fold_in(seeds[1], 1), 0, CLASSES - 1).astype(jnp.int32)
    traces = scatter_about(seeds[2], (GROUPS, N_SUB, STEPS, NY, NZ), 1.0, 6.0, ((0, 4), (1, 64)), jnp.float32)
    new_guess = scatter_about(seeds[3], (TICKS - 1, N_SUB, STEPS, NY, NZ), 1.0, 6.0, ((1, 64),), jnp.float32)
    cond_table = jnp.clip(jnp.exp(jax.random.uniform(seeds[4], (CLASSES,), jnp.float32, math.log(0.2), math.log(5.0))), 0.2, 5.0)
    cap_table = jnp.clip(jnp.exp(jax.random.uniform(seeds[5], (CLASSES,), jnp.float32, math.log(0.5), math.log(4.0))), 0.5, 4.0)
    return {"fields": fields, "labels": labels, "traces": traces, "new_guess": new_guess, "cond_table": cond_table, "cap_table": cap_table}


def harmonic(first, second):
    return 2.0 * first * second / (first + second)


def setup(labels, cond_table, cap_table, left_mask, right_mask):
    conduct = jnp.zeros(labels.shape, jnp.float32)
    capacity = jnp.zeros(labels.shape, jnp.float32)
    for cls in range(cond_table.shape[0]):
        hit = labels == cls
        conduct = jnp.where(hit, cond_table[cls], conduct)
        capacity = jnp.where(hit, cap_table[cls], capacity)
    face_x = harmonic(conduct[:, 1:], conduct[:, :-1])
    face_y = harmonic(conduct[:, :, 1:], conduct[:, :, :-1])
    face_z = harmonic(conduct[:, :, :, 1:], conduct[:, :, :, :-1])
    end_first = 2.0 * conduct[:, 0]
    end_last = 2.0 * conduct[:, -1]
    sum_x = jnp.pad(face_x, ((0, 0), (1, 0), (0, 0), (0, 0))) + jnp.pad(face_x, ((0, 0), (0, 1), (0, 0), (0, 0)))
    sum_x = sum_x.at[:, 0].add(end_first).at[:, -1].add(end_last)
    sum_y = jnp.pad(face_y, ((0, 0), (0, 0), (1, 0), (0, 0))) + jnp.pad(face_y, ((0, 0), (0, 0), (0, 1), (0, 0)))
    sum_y = sum_y.at[:, :, 0].add(2.0 * conduct[:, :, 0]).at[:, :, -1].add(2.0 * conduct[:, :, -1])
    sum_z = jnp.pad(face_z, ((0, 0), (0, 0), (0, 0), (1, 0))) + jnp.pad(face_z, ((0, 0), (0, 0), (0, 0), (0, 1)))
    sum_z = sum_z.at[:, :, :, 0].add(2.0 * conduct[:, :, :, 0]).at[:, :, :, -1].add(2.0 * conduct[:, :, :, -1])
    diag_d = capacity + sum_x + sum_y + sum_z
    diag_n = diag_d.at[:, 0].add(-left_mask[:, None, None] * end_first)
    diag_n = diag_n.at[:, -1].add(-right_mask[:, None, None] * end_last)
    return capacity, face_x, face_y, face_z, end_first, end_last, diag_d, diag_n


def relax(value, rhs, diag, face_x, face_y, face_z):
    for sweep in range(SWEEPS):
        near = jnp.pad(face_x * value[:, :-1], ((0, 0), (1, 0), (0, 0), (0, 0)))
        near = near + jnp.pad(face_x * value[:, 1:], ((0, 0), (0, 1), (0, 0), (0, 0)))
        near = near + jnp.pad(face_y * value[:, :, :-1], ((0, 0), (0, 0), (1, 0), (0, 0)))
        near = near + jnp.pad(face_y * value[:, :, 1:], ((0, 0), (0, 0), (0, 1), (0, 0)))
        near = near + jnp.pad(face_z * value[:, :, :, :-1], ((0, 0), (0, 0), (0, 0), (1, 0)))
        near = near + jnp.pad(face_z * value[:, :, :, 1:], ((0, 0), (0, 0), (0, 0), (0, 1)))
        value = (rhs + near) / diag
    return value


def dirichlet(state, left_trace, right_trace, coeffs):
    capacity, face_x, face_y, face_z, end_first, end_last, diag_d, diag_n = coeffs
    firsts = []
    lasts = []
    for step in range(left_trace.shape[1]):
        rhs = capacity * state
        rhs = rhs.at[:, 0].add(end_first * left_trace[:, step])
        rhs = rhs.at[:, -1].add(end_last * right_trace[:, step])
        state = relax(state, rhs, diag_d, face_x, face_y, face_z)
        firsts.append(state[:, 0])
        lasts.append(state[:, -1])
    return state, jnp.stack(firsts, axis=1), jnp.stack(lasts, axis=1)


def neumann(left_jump, right_jump, coeffs):
    capacity, face_x, face_y, face_z, end_first, end_last, diag_d, diag_n = coeffs
    psi = jnp.zeros(diag_n.shape, jnp.float32)
    firsts = []
    lasts = []
    for step in range(left_jump.shape[1]):
        rhs = capacity * psi
        rhs = rhs.at[:, 0].add(left_jump[:, step])
        rhs = rhs.at[:, -1].add(right_jump[:, step])
        psi = relax(psi, rhs, diag_n, face_x, face_y, face_z)
        firsts.append(psi[:, 0])
        lasts.append(psi[:, -1])
    return jnp.stack(firsts, axis=1), jnp.stack(lasts, axis=1)


def shift_right(planes):
    return jnp.concatenate([jnp.zeros_like(planes[:1]), planes[:-1]], axis=0)


def shift_left(planes):
    return jnp.concatenate([planes[1:], jnp.zeros_like(planes[:1])], axis=0)


def reference(fields, labels, traces, new_guess, cond_table, cap_table):
    slabs = N_SUB
    slab_pos = jnp.arange(slabs)
    left_mask = (slab_pos > 0).astype(jnp.float32)
    right_mask = (slab_pos < slabs - 1).astype(jnp.float32)
    right_wide = right_mask[:, None, None, None]
    coeffs = setup(labels.reshape(slabs, CX, NY, NZ), cond_table, cap_table, left_mask, right_mask)
    end_first, end_last = coeffs[4], coeffs[5]
    states = [fields[group].reshape(slabs, CX, NY, NZ) for group in range(GROUPS)]
    rights = [traces[group] * right_wide for group in range(GROUPS)]
    results = []
    for tick in range(TICKS):
        results = []
        for group in range(GROUPS):
            right_trace = rights[group]
            left_trace = shift_right(right_trace)
            state, firsts, lasts = dirichlet(states[group], left_trace, right_trace, coeffs)
            states[group] = state
            q_first = end_first[:, None] * (firsts - left_trace)
            q_last = end_last[:, None] * (lasts - right_trace)
            right_jump = (q_last + shift_left(q_first)) * right_wide
            left_jump = shift_right(right_jump)
            psi_first, psi_last = neumann(left_jump, right_jump, coeffs)
            results.append((right_trace + 0.25 * (psi_last + shift_left(psi_first))) * right_wide)
        if tick + 1 < TICKS:
            rights = [new_guess[tick] * right_wide] + results[:-1]
    end_fields = jnp.stack([state.reshape(NX, NY, NZ) for state in states])
    return end_fields, jnp.stack(results)
```

```python
import functools

import jax
import jax.numpy as jnp
from jax import lax
from jax.experimental import pallas as pl
from jax.experimental.pallas import tpu as pltpu
from jax.sharding import PartitionSpec as P

MESH = pl.DeviceIdType.MESH
TICKS = 3
STEPS = 4
NY = 128
NZ = 128
PAD = 8
ROWS = NY + 2 * PAD
CHUNK = 32
F32 = jnp.float32


def harmonic(first, second):
    return 2.0 * first * second / (first + second)


def sweep(source, target, rhs, coeff, extra=None):
    for plane in range(2):
        for row in range(0, NY, CHUNK):
            here = slice(row, row + CHUNK)
            base = PAD + row
            v = source[plane, base : base + CHUNK, :]
            out = rhs[plane, here, :]
            out = out + coeff[0, plane, here, :] * source[1 - plane, base : base + CHUNK, :]
            out = out + coeff[1, plane, here, :] * source[plane, base - 1 : base - 1 + CHUNK, :]
            out = out + coeff[2, plane, here, :] * source[plane, base + 1 : base + 1 + CHUNK, :]
            out = out + coeff[3, plane, here, :] * pltpu.roll(v, 1, 1)
            out = out + coeff[4, plane, here, :] * pltpu.roll(v, NZ - 1, 1)
            target[plane, base : base + CHUNK, :] = out
            if extra is not None:
                extra(plane, here, out)


def kernel(
    cond_ref, cap_ref, fields, labels, traces, guess,
    out_u, out_h,
    stage_lab, stage_u, stage_h, lab, u, h_right, h_left, guess_right, guess_left,
    psi, buf_a, buf_b, rhs, co_d, co_n, end, inv_n,
    qf, ql, q_left, q_right, pf, plast, p_left, p_right, back,
    lab_sem, u_sem, h_sem, hl_sem, gr_sem, gl_sem,
    q_sem, p_sem, out_sem, load_sem, send_sem, qs_sem, ps_sem, hs_sem, bs_sem,
):
    sub = lax.axis_index("sub")
    it = lax.axis_index("iter")
    pair = sub // 2
    xl = sub % 2
    xh = it // 2
    core = it % 2
    ring = 2 * xh + xl
    slab = 2 * pair + core
    pairs = lax.axis_size("sub") // 2
    has_left = slab > 0
    has_right = slab < 2 * pairs - 1
    swapped = xl != core
    stays = xl == core
    takes_guess = xh == 1

    right_id = {"sub": sub + 2 * core, "iter": it + 1 - 2 * core}
    left_id = {"sub": sub - 2 * (1 - core), "iter": it + 1 - 2 * core}
    partner_id = {"sub": sub + 1 - 2 * xl, "iter": it + 1 - 2 * core}
    down = (ring + 3) % 4
    up = (ring + 1) % 4
    down_id = {"sub": 2 * pair + down % 2, "iter": 2 * (down // 2) + core}
    up_id = {"sub": 2 * pair + up % 2, "iter": 2 * (up // 2) + core}
    home_id = {"sub": 2 * pair + core, "iter": (ring + 2) % 4}
    source_ring = (it + 2) % 4
    source_id = {"sub": 2 * pair + source_ring % 2, "iter": 2 * (source_ring // 2) + xl}

    def remote(src, dst, send, recv, device):
        return pltpu.make_async_remote_copy(
            src_ref=src, dst_ref=dst, send_sem=send, recv_sem=recv, device_id=device, device_id_type=MESH
        )

    inner = pl.ds(PAD, NY)

    zero_pad = jnp.zeros((2, PAD, NZ), F32)
    for ref in (buf_a, buf_b, psi):
        ref[:, 0:PAD, :] = zero_pad
        ref[:, PAD + NY : ROWS, :] = zero_pad
    for tick in range(TICKS):
        u[tick, :, 0:PAD, :] = zero_pad
        u[tick, :, PAD + NY : ROWS, :] = zero_pad

    barrier = pltpu.get_barrier_semaphore()

    def greet(device):
        pl.semaphore_signal(barrier, inc=1, device_id=device, device_id_type=MESH)

    pl.when(has_left)(lambda: greet(left_id))
    pl.when(has_right)(lambda: greet(right_id))
    pl.when(swapped)(lambda: greet(partner_id))
    greet(up_id)
    greet(source_id)

    def loads(d_h, d_lab, d_u):
        return [
            pltpu.make_async_copy(traces.at[0, 0], d_h, load_sem.at[0]),
            pltpu.make_async_copy(labels, d_lab, load_sem.at[1]),
            pltpu.make_async_copy(fields.at[0], d_u, load_sem.at[2]),
        ]

    keep = loads(h_right, lab, u.at[0, :, inner, :])
    pass_on = loads(stage_h, stage_lab, stage_u)
    keep_guess = pltpu.make_async_copy(guess.at[1 - xl, 0], guess_right, gr_sem)

    @pl.when(stays)
    def _():
        for copy in keep:
            copy.start()

    @pl.when(swapped)
    def _():
        for copy in pass_on:
            copy.start()

    @pl.when(jnp.logical_and(stays, takes_guess))
    def _():
        keep_guess.start()

    peers = 2 + (xl + core) % 2 + jnp.where(has_left, 1, 0) + jnp.where(has_right, 1, 0)
    pl.semaphore_wait(barrier, peers)

    swap_h = [
        remote(stage_h.at[n], h_right.at[n], send_sem.at[n], h_sem.at[n], partner_id) for n in range(STEPS)
    ]
    swap_lab = remote(stage_lab, lab, send_sem.at[4], lab_sem, partner_id)
    swap_u = remote(stage_u, u.at[0, :, inner, :], send_sem.at[5], u_sem.at[0], partner_id)
    swap_guess = remote(guess.at[xl, 0], guess_right, send_sem.at[6], gr_sem, partner_id)
    pass_guess = remote(guess_right, guess_left, send_sem.at[7], gl_sem, right_id)
    move_u = [
        remote(u.at[t, :, inner, :], u.at[t + 1, :, inner, :], send_sem.at[8 + t], u_sem.at[t + 1], down_id)
        for t in range(TICKS - 1)
    ]
    home_u = remote(u.at[TICKS - 1, :, inner, :], out_u.at[0], send_sem.at[8 + TICKS], out_sem.at[STEPS], home_id)

    def pass_h(n):
        return remote(h_right.at[n], h_left.at[n], hs_sem.at[n], hl_sem.at[n], right_id)

    def send_qf(t, n):
        return remote(qf.at[t, n], q_right.at[t, n], qs_sem.at[t, 0, n], q_sem.at[t, 1, n], left_id)

    def send_ql(t, n):
        return remote(ql.at[t, n], q_left.at[t, n], qs_sem.at[t, 1, n], q_sem.at[t, 0, n], right_id)

    def send_pf(t, n):
        return remote(pf.at[t, n], p_right.at[t, n], ps_sem.at[t, 0, n], p_sem.at[t, 1, n], left_id)

    def send_pl(t, n):
        return remote(plast.at[t, n], p_left.at[t, n], ps_sem.at[t, 1, n], p_sem.at[t, 0, n], right_id)

    def send_home(n):
        return remote(back.at[n], out_h.at[0, 0, n], bs_sem.at[n], out_sem.at[n], home_id)

    @pl.when(swapped)
    def _():
        pass_on[0].wait()
        for copy in swap_h:
            copy.start()
        pass_on[1].wait()
        swap_lab.start()
        pass_on[2].wait()
        swap_u.start()

    @pl.when(jnp.logical_and(swapped, takes_guess))
    def _():
        swap_guess.start()

    @pl.when(stays)
    def _():
        keep[0].wait()

    for n in range(STEPS):
        pl.when(swapped)(swap_h[n].wait_recv)
        pl.when(has_right)(pass_h(n).start)

    @pl.when(jnp.logical_not(has_right))
    def _():
        h_right[...] = jnp.zeros((STEPS, NY, NZ), F32)

    @pl.when(jnp.logical_not(has_left))
    def _():
        h_left[...] = jnp.zeros((STEPS, NY, NZ), F32)

    pl.when(stays)(keep[1].wait)
    pl.when(swapped)(swap_lab.wait_recv)

    def pick(table, value):
        result = jnp.full(value.shape, table[0], F32)
        for cls in range(1, 4):
            result = jnp.where(value == cls, table[cls], result)
        return result

    for plane in range(2):
        for row in range(0, NY, CHUNK):
            buf_a[plane, PAD + row : PAD + row + CHUNK, :] = pick(cond_ref, lab[plane, row : row + CHUNK, :])
    lane = lax.broadcasted_iota(jnp.int32, (CHUNK, NZ), 1)
    line = lax.broadcasted_iota(jnp.int32, (CHUNK, NZ), 0)
    for plane in range(2):
        edge = has_left if plane == 0 else has_right
        for row in range(0, NY, CHUNK):
            here = slice(row, row + CHUNK)
            base = PAD + row
            k = buf_a[plane, base : base + CHUNK, :]
            twice = 2.0 * k
            face_x = harmonic(k, buf_a[1 - plane, base : base + CHUNK, :])
            face_u = harmonic(k, buf_a[plane, base - 1 : base - 1 + CHUNK, :])
            face_d = harmonic(k, buf_a[plane, base + 1 : base + 1 + CHUNK, :])
            face_l = jnp.where(lane == 0, 0.0, harmonic(k, pltpu.roll(k, 1, 1)))
            face_r = jnp.where(lane == NZ - 1, 0.0, harmonic(k, pltpu.roll(k, NZ - 1, 1)))
            side_u = jnp.where(line + row == 0, twice, face_u) if row == 0 else face_u
            side_d = jnp.where(line + row == NY - 1, twice, face_d) if row + CHUNK == NY else face_d
            side_l = jnp.where(lane == 0, twice, face_l)
            side_r = jnp.where(lane == NZ - 1, twice, face_r)
            capacity = pick(cap_ref, lab[plane, here, :])
            common = capacity + face_x + side_u + side_d + side_l + side_r
            inv_dir = 1.0 / (common + twice)
            inv_neu = 1.0 / jnp.where(edge, common, common + twice)
            faces = (face_x, face_u, face_d, face_l, face_r, capacity)
            for j, face in enumerate(faces):
                co_d[j, plane, here, :] = face * inv_dir
                co_n[j, plane, here, :] = face * inv_neu
            co_d[6, plane, here, :] = twice * inv_dir
            end[plane, here, :] = twice
            inv_n[plane, here, :] = inv_neu

    pl.when(stays)(keep[2].wait)
    pl.when(swapped)(swap_u.wait_recv)

    for tick in range(TICKS):
        state = u.at[tick]
        if tick > 0:
            restart = ring == (4 - tick)
            restart_r = jnp.logical_and(restart, has_right)
            restart_l = jnp.logical_and(restart, has_left)
            move_u[tick - 1].wait_recv()
            if tick == 1:
                pl.when(jnp.logical_and(takes_guess, has_left))(pass_guess.wait_recv)

        def dirichlet(n, carry, tick=tick, state=state):
            if tick == 0:
                pl.when(has_left)(pass_h(n).wait_recv)
            else:
                pl.when(has_right)(send_pf(tick - 1, n).wait_recv)
                pl.when(has_left)(send_pl(tick - 1, n).wait_recv)
                if tick == 1:
                    pl.when(has_right)(pass_h(n).wait_send)
                for row in range(0, NY, CHUNK):
                    here = slice(row, row + CHUNK)
                    old = h_right[n, here, :]
                    new = old + 0.25 * (plast[tick - 1, n, here, :] + p_right[tick - 1, n, here, :])
                    new = jnp.where(has_right, new, 0.0)
                    h_right[n, here, :] = jnp.where(restart_r, guess_right[n, here, :], new)
                    old = h_left[n, here, :]
                    new = old + 0.25 * (p_left[tick - 1, n, here, :] + pf[tick - 1, n, here, :])
                    new = jnp.where(has_left, new, 0.0)
                    h_left[n, here, :] = jnp.where(restart_l, guess_left[n, here, :], new)
            for plane, trace in enumerate((h_left, h_right)):
                for row in range(0, NY, CHUNK):
                    here = slice(row, row + CHUNK)
                    rhs[plane, here, :] = (
                        co_d[5, plane, here, :] * state[plane, PAD + row : PAD + row + CHUNK, :]
                        + co_d[6, plane, here, :] * trace[n, here, :]
                    )

            def flux(plane, here, value):
                if plane == 0:
                    qf[tick, n, here, :] = end[0, here, :] * (value - h_left[n, here, :])
                else:
                    ql[tick, n, here, :] = end[1, here, :] * (value - h_right[n, here, :])

            sweep(state, buf_a, rhs, co_d)
            sweep(buf_a, buf_b, rhs, co_d)
            sweep(buf_b, state, rhs, co_d, flux)
            pl.when(has_right)(send_ql(tick, n).start)
            pl.when(has_left)(send_qf(tick, n).start)
            return carry

        lax.fori_loop(0, STEPS, dirichlet, 0)
        if tick + 1 < TICKS:
            move_u[tick].start()
        else:
            home_u.start()
        if tick == 0:

            @pl.when(takes_guess)
            def _():
                pl.when(stays)(keep_guess.wait)
                pl.when(swapped)(swap_guess.wait_recv)
                pl.when(has_right)(pass_guess.start)

        def neumann(n, carry, tick=tick, first=False):
            pl.when(has_right)(send_qf(tick, n).wait_recv)
            pl.when(has_left)(send_ql(tick, n).wait_recv)
            for plane in range(2):
                own, got, edge = ((qf, q_left, has_left), (ql, q_right, has_right))[plane]
                for row in range(0, NY, CHUNK):
                    here = slice(row, row + CHUNK)
                    jump = own[tick, n, here, :] + got[tick, n, here, :]
                    value = inv_n[plane, here, :] * jnp.where(edge, jump, 0.0)
                    if not first:
                        value = value + co_n[5, plane, here, :] * psi[plane, PAD + row : PAD + row + CHUNK, :]
                    rhs[plane, here, :] = value
                    if first:
                        buf_a[plane, PAD + row : PAD + row + CHUNK, :] = value

            def ends(plane, here, value):
                (pf, plast)[plane][tick, n, here, :] = value

            if not first:
                sweep(psi, buf_a, rhs, co_n)
            sweep(buf_a, buf_b, rhs, co_n)
            sweep(buf_b, psi, rhs, co_n, ends)
            pl.when(has_left)(send_pf(tick, n).start)
            if tick + 1 < TICKS:
                pl.when(has_right)(send_pl(tick, n).start)
            return carry

        neumann(0, 0, first=True)
        lax.fori_loop(1, STEPS, neumann, 0)

    last = TICKS - 1

    def finish(n, carry):
        pl.when(has_right)(send_pf(last, n).wait_recv)
        for row in range(0, NY, CHUNK):
            here = slice(row, row + CHUNK)
            new = h_right[n, here, :] + 0.25 * (plast[last, n, here, :] + p_right[last, n, here, :])
            back[n, here, :] = jnp.where(has_right, new, 0.0)
        send_home(n).start()
        return carry

    lax.fori_loop(0, STEPS, finish, 0)

    @pl.when(swapped)
    def _():
        for copy in swap_h:
            copy.wait_send()
        swap_lab.wait_send()
        swap_u.wait_send()

    pl.when(jnp.logical_and(swapped, takes_guess))(swap_guess.wait_send)
    pl.when(jnp.logical_and(takes_guess, has_right))(pass_guess.wait_send)
    for copy in move_u:
        copy.wait_send()
    home_u.wait_send()

    @pl.when(has_right)
    def _():
        for n in range(STEPS):
            for t in range(TICKS):
                send_ql(t, n).wait_send()
                if t < last:
                    send_pl(t, n).wait_send()

    @pl.when(has_left)
    def _():
        for n in range(STEPS):
            for t in range(TICKS):
                send_qf(t, n).wait_send()
                send_pf(t, n).wait_send()

    for n in range(STEPS):
        send_home(n).wait_send()
    home_u.wait_recv()
    for n in range(STEPS):
        send_home(n).wait_recv()


def local(fields, labels, traces, new_guess, cond_table, cap_table):
    plane = (NY, NZ)
    field = (2, ROWS, NZ)
    vm = lambda *shape: pltpu.VMEM(shape, F32)
    dma = lambda *shape: pltpu.SemaphoreType.DMA(shape)
    any_spec = pl.BlockSpec(memory_space=pl.ANY)
    smem = pl.BlockSpec(memory_space=pltpu.SMEM)
    per_step = (TICKS, STEPS) + plane
    return pl.pallas_call(
        kernel,
        out_shape=(
            jax.ShapeDtypeStruct((1, 2) + plane, F32),
            jax.ShapeDtypeStruct((1, 1, STEPS) + plane, F32),
        ),
        in_specs=[smem, smem, any_spec, any_spec, any_spec, any_spec],
        out_specs=(any_spec, any_spec),
        scratch_shapes=[
            pltpu.VMEM((2,) + plane, jnp.int32),
            vm(2, *plane),
            vm(STEPS, *plane),
            pltpu.VMEM((2,) + plane, jnp.int32),
            vm(TICKS, *field),
            vm(STEPS, *plane),
            vm(STEPS, *plane),
            vm(STEPS, *plane),
            vm(STEPS, *plane),
            vm(*field),
            vm(*field),
            vm(*field),
            vm(2, *plane),
            vm(7, 2, *plane),
            vm(6, 2, *plane),
            vm(2, *plane),
            vm(2, *plane),
            vm(*per_step),
            vm(*per_step),
            vm(*per_step),
            vm(*per_step),
            vm(*per_step),
            vm(*per_step),
            vm(*per_step),
            vm(*per_step),
            vm(STEPS, *plane),
            pltpu.SemaphoreType.DMA,
            dma(TICKS),
            dma(STEPS),
            dma(STEPS),
            pltpu.SemaphoreType.DMA,
            pltpu.SemaphoreType.DMA,
            dma(TICKS, 2, STEPS),
            dma(TICKS, 2, STEPS),
            dma(STEPS + 1),
            dma(3),
            dma(8 + TICKS + 1),
            dma(TICKS, 2, STEPS),
            dma(TICKS, 2, STEPS),
            dma(STEPS),
            dma(STEPS),
        ],
        compiler_params=pltpu.CompilerParams(collective_id=0, has_side_effects=True),
    )(cond_table, cap_table, fields, labels, traces, new_guess)


def solution(mesh):
    return jax.shard_map(
        local,
        mesh=mesh,
        in_specs=(
            P("iter", "sub", None, None),
            P("sub", None, None),
            P("iter", "sub", None, None, None),
            P(None, "sub", None, None, None),
            P(),
            P(),
        ),
        out_specs=(P("iter", "sub", None, None), P("iter", "sub", None, None, None)),
        check_vma=False,
    )
```

```python
import functools

import jax
import jax.numpy as jnp
from jax import lax
from jax.experimental import pallas as pl
from jax.experimental.pallas import tpu as pltpu
from jax.sharding import PartitionSpec as P

MESH = pl.DeviceIdType.MESH
TICKS = 3
STEPS = 4
NY = 128
NZ = 128
PAD = 8
ROWS = NY + 2 * PAD
CHUNK = 32
F32 = jnp.float32


def harmonic(first, second):
    return 2.0 * first * second / (first + second)


def sweep(source, target, rhs, coeff, extra=None):
    for plane in range(2):
        for row in range(0, NY, CHUNK):
            here = slice(row, row + CHUNK)
            base = PAD + row
            v = source[plane, base : base + CHUNK, :]
            out = rhs[plane, here, :]
            out = out + coeff[0, plane, here, :] * source[1 - plane, base : base + CHUNK, :]
            out = out + coeff[1, plane, here, :] * source[plane, base - 1 : base - 1 + CHUNK, :]
            out = out + coeff[2, plane, here, :] * source[plane, base + 1 : base + 1 + CHUNK, :]
            out = out + coeff[3, plane, here, :] * pltpu.roll(v, 1, 1)
            out = out + coeff[4, plane, here, :] * pltpu.roll(v, NZ - 1, 1)
            target[plane, base : base + CHUNK, :] = out
            if extra is not None:
                extra(plane, here, out)


def kernel(
    cond_hbm, cap_hbm, fields, labels, traces, guess,
    out_u, out_h,
    cond_ref, cap_ref,
    stage_lab, stage_u, stage_h, lab, u, h_right, h_left, guess_right, guess_left,
    psi, buf_a, buf_b, rhs, co_d, co_n, end, inv_n,
    qf, ql, q_left, q_right, pf, plast, p_left, p_right, back,
    lab_sem, u_sem, h_sem, hl_sem, gr_sem, gl_sem,
    q_sem, p_sem, out_sem, load_sem, send_sem, qs_sem, ps_sem, hs_sem, bs_sem,
):
    sub = lax.axis_index("sub")
    it = lax.axis_index("iter")
    pair = sub // 2
    xl = sub % 2
    xh = it // 2
    core = it % 2
    ring = 2 * xh + xl
    slab = 2 * pair + core
    pairs = lax.axis_size("sub") // 2
    has_left = slab > 0
    has_right = slab < 2 * pairs - 1
    swapped = xl != core
    stays = xl == core
    takes_guess = xh == 1

    right_id = {"sub": sub + 2 * core, "iter": it + 1 - 2 * core}
    left_id = {"sub": sub - 2 * (1 - core), "iter": it + 1 - 2 * core}
    partner_id = {"sub": sub + 1 - 2 * xl, "iter": it + 1 - 2 * core}
    down = (ring + 3) % 4
    up = (ring + 1) % 4
    down_id = {"sub": 2 * pair + down % 2, "iter": 2 * (down // 2) + core}
    up_id = {"sub": 2 * pair + up % 2, "iter": 2 * (up // 2) + core}
    other = (ring + 1 + 2 * core) % 4
    other_id = {"sub": 2 * pair + other % 2, "iter": 2 * (other // 2) + 1 - core}
    home_id = {"sub": 2 * pair + core, "iter": (ring + 2) % 4}
    source_ring = (it + 2) % 4
    source_id = {"sub": 2 * pair + source_ring % 2, "iter": 2 * (source_ring // 2) + xl}

    def remote(src, dst, send, recv, device):
        return pltpu.make_async_remote_copy(
            src_ref=src, dst_ref=dst, send_sem=send, recv_sem=recv, device_id=device, device_id_type=MESH
        )

    inner = pl.ds(PAD, NY)

    zero_pad = jnp.zeros((2, PAD, NZ), F32)
    for ref in (buf_a, buf_b, psi):
        ref[:, 0:PAD, :] = zero_pad
        ref[:, PAD + NY : ROWS, :] = zero_pad
    for tick in range(TICKS):
        u[tick, :, 0:PAD, :] = zero_pad
        u[tick, :, PAD + NY : ROWS, :] = zero_pad

    barrier = pltpu.get_barrier_semaphore()

    def greet(device):
        pl.semaphore_signal(barrier, inc=1, device_id=device, device_id_type=MESH)

    pl.when(has_left)(lambda: greet(left_id))
    pl.when(has_right)(lambda: greet(right_id))
    pl.when(swapped)(lambda: greet(partner_id))
    pl.when(swapped)(lambda: greet(other_id))
    greet(up_id)
    greet(source_id)

    def loads(d_h, d_lab, d_u):
        return [
            pltpu.make_async_copy(traces.at[0, 0, 0:1], d_h.at[0:1], load_sem.at[0]),
            pltpu.make_async_copy(labels, d_lab, load_sem.at[1]),
            pltpu.make_async_copy(fields.at[0], d_u, load_sem.at[2]),
            pltpu.make_async_copy(traces.at[0, 0, 1:STEPS], d_h.at[1:STEPS], load_sem.at[3]),
        ]

    keep = loads(h_right, lab, u.at[0, :, inner, :])
    pass_on = loads(stage_h, stage_lab, stage_u)
    keep_guess = pltpu.make_async_copy(guess.at[1 - xl, 0], guess_right, gr_sem)

    tables = [
        pltpu.make_async_copy(cond_hbm, cond_ref, load_sem.at[4]),
        pltpu.make_async_copy(cap_hbm, cap_ref, load_sem.at[5]),
    ]
    for copy in tables:
        copy.start()

    @pl.when(stays)
    def _():
        for copy in keep:
            copy.start()

    @pl.when(swapped)
    def _():
        for copy in pass_on:
            copy.start()

    @pl.when(jnp.logical_and(stays, takes_guess))
    def _():
        keep_guess.start()

    peers = 2 + 2 * ((xl + core) % 2) + jnp.where(has_left, 1, 0) + jnp.where(has_right, 1, 0)
    pl.semaphore_wait(barrier, peers)

    swap_h = [
        remote(stage_h.at[n], h_right.at[n], send_sem.at[n], h_sem.at[n], partner_id) for n in range(STEPS)
    ]
    swap_lab = remote(stage_lab, lab, send_sem.at[4], lab_sem, other_id)
    swap_u = remote(stage_u, u.at[0, :, inner, :], send_sem.at[5], u_sem.at[0], partner_id)
    swap_guess = remote(guess.at[xl, 0], guess_right, send_sem.at[6], gr_sem, partner_id)
    pass_guess = remote(guess_right, guess_left, send_sem.at[7], gl_sem, right_id)
    move_u = [
        remote(u.at[t, :, inner, :], u.at[t + 1, :, inner, :], send_sem.at[8 + t], u_sem.at[t + 1], down_id)
        for t in range(TICKS - 1)
    ]
    home_u = remote(u.at[TICKS - 1, :, inner, :], out_u.at[0], send_sem.at[8 + TICKS], out_sem.at[STEPS], home_id)

    def pass_h(n):
        return remote(h_right.at[n], h_left.at[n], hs_sem.at[n], hl_sem.at[n], right_id)

    def send_qf(t, n):
        return remote(qf.at[t, n], q_right.at[t, n], qs_sem.at[t, 0, n], q_sem.at[t, 1, n], left_id)

    def send_ql(t, n):
        return remote(ql.at[t, n], q_left.at[t, n], qs_sem.at[t, 1, n], q_sem.at[t, 0, n], right_id)

    def send_pf(t, n):
        return remote(pf.at[t, n], p_right.at[t, n], ps_sem.at[t, 0, n], p_sem.at[t, 1, n], left_id)

    def send_pl(t, n):
        return remote(plast.at[t, n], p_left.at[t, n], ps_sem.at[t, 1, n], p_sem.at[t, 0, n], right_id)

    def send_home(n):
        return remote(back.at[n], out_h.at[0, 0, n], bs_sem.at[n], out_sem.at[n], home_id)

    @pl.when(swapped)
    def _():
        pass_on[0].wait()
        swap_h[0].start()
        pass_on[1].wait()
        swap_lab.start()
        pass_on[2].wait()
        swap_u.start()
        pass_on[3].wait()
        for copy in swap_h[1:]:
            copy.start()

    @pl.when(jnp.logical_and(swapped, takes_guess))
    def _():
        swap_guess.start()

    @pl.when(stays)
    def _():
        keep[0].wait()

    pl.when(swapped)(swap_h[0].wait_recv)
    pl.when(has_right)(pass_h(0).start)

    @pl.when(stays)
    def _():
        keep[3].wait()
        for n in range(1, STEPS):
            pl.when(has_right)(pass_h(n).start)

    nothing = jnp.zeros((NY, NZ), F32)

    @pl.when(jnp.logical_not(has_right))
    def _():
        h_right[0] = nothing
        pl.when(stays)(lambda: h_right.__setitem__(slice(1, STEPS), jnp.zeros((STEPS - 1, NY, NZ), F32)))

    @pl.when(jnp.logical_not(has_left))
    def _():
        h_left[...] = jnp.zeros((STEPS, NY, NZ), F32)

    def pass_next(n):
        @pl.when(jnp.logical_and(swapped, n + 1 < STEPS))
        def _():
            follow = n + 1
            remote(
                stage_h.at[follow], h_right.at[follow], send_sem.at[follow], h_sem.at[follow], partner_id
            ).wait_recv()
            pl.when(has_right)(pass_h(follow).start)

            @pl.when(jnp.logical_not(has_right))
            def _():
                h_right[follow] = nothing

    pl.when(stays)(keep[1].wait)
    pl.when(swapped)(swap_lab.wait_recv)

    for copy in tables:
        copy.wait()

    def pick(table, value):
        result = jnp.full(value.shape, table[0], F32)
        for cls in range(1, 4):
            result = jnp.where(value == cls, table[cls], result)
        return result

    for plane in range(2):
        for row in range(0, NY, CHUNK):
            buf_a[plane, PAD + row : PAD + row + CHUNK, :] = pick(cond_ref, lab[plane, row : row + CHUNK, :])
    lane = lax.broadcasted_iota(jnp.int32, (CHUNK, NZ), 1)
    line = lax.broadcasted_iota(jnp.int32, (CHUNK, NZ), 0)
    for plane in range(2):
        edge = has_left if plane == 0 else has_right
        for row in range(0, NY, CHUNK):
            here = slice(row, row + CHUNK)
            base = PAD + row
            k = buf_a[plane, base : base + CHUNK, :]
            twice = 2.0 * k
            face_x = harmonic(k, buf_a[1 - plane, base : base + CHUNK, :])
            face_u = harmonic(k, buf_a[plane, base - 1 : base - 1 + CHUNK, :])
            face_d = harmonic(k, buf_a[plane, base + 1 : base + 1 + CHUNK, :])
            face_l = jnp.where(lane == 0, 0.0, harmonic(k, pltpu.roll(k, 1, 1)))
            face_r = jnp.where(lane == NZ - 1, 0.0, harmonic(k, pltpu.roll(k, NZ - 1, 1)))
            side_u = jnp.where(line + row == 0, twice, face_u) if row == 0 else face_u
            side_d = jnp.where(line + row == NY - 1, twice, face_d) if row + CHUNK == NY else face_d
            side_l = jnp.where(lane == 0, twice, face_l)
            side_r = jnp.where(lane == NZ - 1, twice, face_r)
            capacity = pick(cap_ref, lab[plane, here, :])
            common = capacity + face_x + side_u + side_d + side_l + side_r
            inv_dir = 1.0 / (common + twice)
            inv_neu = 1.0 / jnp.where(edge, common, common + twice)
            faces = (face_x, face_u, face_d, face_l, face_r, capacity)
            for j, face in enumerate(faces):
                co_d[j, plane, here, :] = face * inv_dir
                co_n[j, plane, here, :] = face * inv_neu
            co_d[6, plane, here, :] = twice * inv_dir
            end[plane, here, :] = twice
            inv_n[plane, here, :] = inv_neu

    pl.when(stays)(keep[2].wait)
    pl.when(swapped)(swap_u.wait_recv)

    for tick in range(TICKS):
        state = u.at[tick]
        if tick > 0:
            restart = ring == (4 - tick)
            restart_r = jnp.logical_and(restart, has_right)
            restart_l = jnp.logical_and(restart, has_left)
            move_u[tick - 1].wait_recv()
            if tick == 1:
                pl.when(jnp.logical_and(takes_guess, has_left))(pass_guess.wait_recv)

        def dirichlet(n, carry, tick=tick, state=state):
            if tick == 0:
                pl.when(has_left)(pass_h(n).wait_recv)
            else:
                pl.when(has_right)(send_pf(tick - 1, n).wait_recv)
                pl.when(has_left)(send_pl(tick - 1, n).wait_recv)
                if tick == 1:
                    pl.when(has_right)(pass_h(n).wait_send)
                for row in range(0, NY, CHUNK):
                    here = slice(row, row + CHUNK)
                    old = h_right[n, here, :]
                    new = old + 0.25 * (plast[tick - 1, n, here, :] + p_right[tick - 1, n, here, :])
                    new = jnp.where(has_right, new, 0.0)
                    h_right[n, here, :] = jnp.where(restart_r, guess_right[n, here, :], new)
                    old = h_left[n, here, :]
                    new = old + 0.25 * (p_left[tick - 1, n, here, :] + pf[tick - 1, n, here, :])
                    new = jnp.where(has_left, new, 0.0)
                    h_left[n, here, :] = jnp.where(restart_l, guess_left[n, here, :], new)
            for plane, trace in enumerate((h_left, h_right)):
                for row in range(0, NY, CHUNK):
                    here = slice(row, row + CHUNK)
                    rhs[plane, here, :] = (
                        co_d[5, plane, here, :] * state[plane, PAD + row : PAD + row + CHUNK, :]
                        + co_d[6, plane, here, :] * trace[n, here, :]
                    )

            def flux(plane, here, value):
                if plane == 0:
                    qf[tick, n, here, :] = end[0, here, :] * (value - h_left[n, here, :])
                else:
                    ql[tick, n, here, :] = end[1, here, :] * (value - h_right[n, here, :])

            sweep(state, buf_a, rhs, co_d)
            sweep(buf_a, buf_b, rhs, co_d)
            sweep(buf_b, state, rhs, co_d, flux)
            pl.when(has_right)(send_ql(tick, n).start)
            pl.when(has_left)(send_qf(tick, n).start)
            if tick == 0:
                pass_next(n)
            return carry

        lax.fori_loop(0, STEPS, dirichlet, 0)
        if tick + 1 < TICKS:
            move_u[tick].start()
        else:
            home_u.start()
        if tick == 0:

            @pl.when(takes_guess)
            def _():
                pl.when(stays)(keep_guess.wait)
                pl.when(swapped)(swap_guess.wait_recv)
                pl.when(has_right)(pass_guess.start)

        def neumann(n, carry, tick=tick, first=False):
            pl.when(has_right)(send_qf(tick, n).wait_recv)
            pl.when(has_left)(send_ql(tick, n).wait_recv)
            for plane in range(2):
                own, got, edge = ((qf, q_left, has_left), (ql, q_right, has_right))[plane]
                for row in range(0, NY, CHUNK):
                    here = slice(row, row + CHUNK)
                    jump = own[tick, n, here, :] + got[tick, n, here, :]
                    value = inv_n[plane, here, :] * jnp.where(edge, jump, 0.0)
                    if not first:
                        value = value + co_n[5, plane, here, :] * psi[plane, PAD + row : PAD + row + CHUNK, :]
                    rhs[plane, here, :] = value
                    if first:
                        buf_a[plane, PAD + row : PAD + row + CHUNK, :] = value

            def ends(plane, here, value):
                (pf, plast)[plane][tick, n, here, :] = value

            if not first:
                sweep(psi, buf_a, rhs, co_n)
            sweep(buf_a, buf_b, rhs, co_n)
            sweep(buf_b, psi, rhs, co_n, ends)
            pl.when(has_left)(send_pf(tick, n).start)
            if tick + 1 < TICKS:
                pl.when(has_right)(send_pl(tick, n).start)
            return carry

        neumann(0, 0, first=True)
        lax.fori_loop(1, STEPS, neumann, 0)

    last = TICKS - 1

    def finish(n, carry):
        pl.when(has_right)(send_pf(last, n).wait_recv)
        for row in range(0, NY, CHUNK):
            here = slice(row, row + CHUNK)
            new = h_right[n, here, :] + 0.25 * (plast[last, n, here, :] + p_right[last, n, here, :])
            back[n, here, :] = jnp.where(has_right, new, 0.0)
        send_home(n).start()
        return carry

    lax.fori_loop(0, STEPS, finish, 0)

    @pl.when(swapped)
    def _():
        for copy in swap_h:
            copy.wait_send()
        swap_lab.wait_send()
        swap_u.wait_send()

    pl.when(jnp.logical_and(swapped, takes_guess))(swap_guess.wait_send)
    pl.when(jnp.logical_and(takes_guess, has_right))(pass_guess.wait_send)
    for copy in move_u:
        copy.wait_send()
    home_u.wait_send()

    @pl.when(has_right)
    def _():
        for n in range(STEPS):
            for t in range(TICKS):
                send_ql(t, n).wait_send()
                if t < last:
                    send_pl(t, n).wait_send()

    @pl.when(has_left)
    def _():
        for n in range(STEPS):
            for t in range(TICKS):
                send_qf(t, n).wait_send()
                send_pf(t, n).wait_send()

    for n in range(STEPS):
        send_home(n).wait_send()
    home_u.wait_recv()
    for n in range(STEPS):
        send_home(n).wait_recv()


def local(fields, labels, traces, new_guess, cond_table, cap_table):
    plane = (NY, NZ)
    field = (2, ROWS, NZ)
    vm = lambda *shape: pltpu.VMEM(shape, F32)
    dma = lambda *shape: pltpu.SemaphoreType.DMA(shape)
    any_spec = pl.BlockSpec(memory_space=pl.ANY)
    hbm = pl.BlockSpec(memory_space=pltpu.HBM)
    per_step = (TICKS, STEPS) + plane
    return pl.pallas_call(
        kernel,
        out_shape=(
            jax.ShapeDtypeStruct((1, 2) + plane, F32),
            jax.ShapeDtypeStruct((1, 1, STEPS) + plane, F32),
        ),
        in_specs=[hbm] * 6,
        out_specs=(any_spec, any_spec),
        scratch_shapes=[
            pltpu.SMEM((4,), F32),
            pltpu.SMEM((4,), F32),
            pltpu.VMEM((2,) + plane, jnp.int32),
            vm(2, *plane),
            vm(STEPS, *plane),
            pltpu.VMEM((2,) + plane, jnp.int32),
            vm(TICKS, *field),
            vm(STEPS, *plane),
            vm(STEPS, *plane),
            vm(STEPS, *plane),
            vm(STEPS, *plane),
            vm(*field),
            vm(*field),
            vm(*field),
            vm(2, *plane),
            vm(7, 2, *plane),
            vm(6, 2, *plane),
            vm(2, *plane),
            vm(2, *plane),
            vm(*per_step),
            vm(*per_step),
            vm(*per_step),
            vm(*per_step),
            vm(*per_step),
            vm(*per_step),
            vm(*per_step),
            vm(*per_step),
            vm(STEPS, *plane),
            pltpu.SemaphoreType.DMA,
            dma(TICKS),
            dma(STEPS),
            dma(STEPS),
            pltpu.SemaphoreType.DMA,
            pltpu.SemaphoreType.DMA,
            dma(TICKS, 2, STEPS),
            dma(TICKS, 2, STEPS),
            dma(STEPS + 1),
            dma(6),
            dma(8 + TICKS + 1),
            dma(TICKS, 2, STEPS),
            dma(TICKS, 2, STEPS),
            dma(STEPS),
            dma(STEPS),
        ],
        compiler_params=pltpu.CompilerParams(collective_id=0, has_side_effects=True, vmem_limit_bytes=24 * 2**20),
    )(cond_table, cap_table, fields, labels, traces, new_guess)


def solution(mesh):
    return jax.shard_map(
        local,
        mesh=mesh,
        in_specs=(
            P("iter", "sub", None, None),
            P("sub", None, None),
            P("iter", "sub", None, None, None),
            P(None, "sub", None, None, None),
            P(),
            P(),
        ),
        out_specs=(P("iter", "sub", None, None), P("iter", "sub", None, None, None)),
        check_vma=False,
    )
```

```python
import functools

import jax
import jax.numpy as jnp
from jax import lax
from jax.experimental import pallas as pl
from jax.experimental.pallas import tpu as pltpu
from jax.sharding import PartitionSpec as P

MESH = pl.DeviceIdType.MESH
TICKS = 3
STEPS = 4
NY = 128
NZ = 128
PAD = 8
ROWS = NY + 2 * PAD
CHUNK = 32
SPAN = 8
F32 = jnp.float32


def harmonic(first, second):
    return 2.0 * first * second / (first + second)


def sweep(source, target, rhs, coeff, extra=None):
    for plane in range(2):
        for row in range(0, NY, CHUNK):
            here = slice(row, row + CHUNK)
            base = PAD + row
            v = source[plane, base : base + CHUNK, :]
            out = rhs[plane, here, :]
            out = out + coeff[0, plane, here, :] * source[1 - plane, base : base + CHUNK, :]
            out = out + coeff[1, plane, here, :] * source[plane, base - 1 : base - 1 + CHUNK, :]
            out = out + coeff[2, plane, here, :] * source[plane, base + 1 : base + 1 + CHUNK, :]
            out = out + coeff[3, plane, here, :] * pltpu.roll(v, 1, 1)
            out = out + coeff[4, plane, here, :] * pltpu.roll(v, NZ - 1, 1)
            target[plane, base : base + CHUNK, :] = out
            if extra is not None:
                extra(plane, here, out)


def kernel(
    cond_hbm, cap_hbm, fields, labels, traces, guess,
    out_u, out_h,
    cond_ref, cap_ref,
    stage_lab, stage_u, stage_h, lab, u, h_right, h_left, guess_right, guess_left,
    psi, buf_a, buf_b, rhs, co_d, co_n, end, inv_n,
    qs, qr, ps, pr, back,
    lab_o, co_o, inv_o, psi_o, jump_in, jump_far,
    lab_sem, u_sem, h_sem, hl_sem, gr_sem, gl_sem,
    q_sem, p_sem, out_sem, load_sem, send_sem, qs_sem, ps_sem, hs_sem, bs_sem,
    lab_o_sem, far_sem, in_sem,
):
    sub = lax.axis_index("sub")
    it = lax.axis_index("iter")
    pair = sub // 2
    xl = sub % 2
    xh = it // 2
    core = it % 2
    ring = 2 * xh + xl
    slab = 2 * pair + core
    pairs = lax.axis_size("sub") // 2
    has_left = slab > 0
    has_right = slab < 2 * pairs - 1
    swapped = xl != core
    stays = xl == core
    takes_guess = xh == 1

    outer_right = jnp.logical_and(jnp.logical_and(core == 1, has_right), pair % SPAN == SPAN - 1)
    outer_left = jnp.logical_and(jnp.logical_and(core == 0, has_left), pair % SPAN == 0)
    long = jnp.logical_or(outer_right, outer_left)
    short = jnp.logical_not(long)
    exists = (has_left, has_right)
    restart = [None] + [ring == 4 - tick for tick in range(1, TICKS)]
    useful = [ring != 3 - tick for tick in range(TICKS - 1)] + [ring >= 0]
    q_wait = (
        jnp.logical_and(has_left, jnp.logical_not(outer_right)),
        jnp.logical_and(has_right, jnp.logical_not(outer_left)),
    )
    p_uses = (
        jnp.logical_and(has_left, jnp.logical_not(outer_left)),
        jnp.logical_and(has_right, jnp.logical_not(outer_right)),
    )
    outer_id = {"sub": sub + 4 * core - 2, "iter": it + 1 - 2 * core}

    right_id = {"sub": sub + 2 * core, "iter": it + 1 - 2 * core}
    left_id = {"sub": sub - 2 * (1 - core), "iter": it + 1 - 2 * core}
    partner_id = {"sub": sub + 1 - 2 * xl, "iter": it + 1 - 2 * core}
    down = (ring + 3) % 4
    up = (ring + 1) % 4
    down_id = {"sub": 2 * pair + down % 2, "iter": 2 * (down // 2) + core}
    up_id = {"sub": 2 * pair + up % 2, "iter": 2 * (up // 2) + core}
    other = (ring + 1 + 2 * core) % 4
    other_id = {"sub": 2 * pair + other % 2, "iter": 2 * (other // 2) + 1 - core}
    home_id = {"sub": 2 * pair + core, "iter": (ring + 2) % 4}
    source_ring = (it + 2) % 4
    source_id = {"sub": 2 * pair + source_ring % 2, "iter": 2 * (source_ring // 2) + xl}

    def remote(src, dst, send, recv, device):
        return pltpu.make_async_remote_copy(
            src_ref=src, dst_ref=dst, send_sem=send, recv_sem=recv, device_id=device, device_id_type=MESH
        )

    inner = pl.ds(PAD, NY)

    zero_pad = jnp.zeros((2, PAD, NZ), F32)
    for ref in (buf_a, buf_b, psi, psi_o):
        ref[:, 0:PAD, :] = zero_pad
        ref[:, PAD + NY : ROWS, :] = zero_pad
    for tick in range(TICKS):
        u[tick, :, 0:PAD, :] = zero_pad
        u[tick, :, PAD + NY : ROWS, :] = zero_pad

    barrier = pltpu.get_barrier_semaphore()

    def greet(device):
        pl.semaphore_signal(barrier, inc=1, device_id=device, device_id_type=MESH)

    pl.when(has_left)(lambda: greet(left_id))
    pl.when(has_right)(lambda: greet(right_id))
    pl.when(swapped)(lambda: greet(partner_id))
    pl.when(swapped)(lambda: greet(other_id))
    greet(up_id)
    greet(source_id)

    def loads(d_h, d_lab, d_u):
        return [
            pltpu.make_async_copy(traces.at[0, 0, 0:1], d_h.at[0:1], load_sem.at[0]),
            pltpu.make_async_copy(labels, d_lab, load_sem.at[1]),
            pltpu.make_async_copy(fields.at[0], d_u, load_sem.at[2]),
            pltpu.make_async_copy(traces.at[0, 0, 1:STEPS], d_h.at[1:STEPS], load_sem.at[3]),
        ]

    keep = loads(h_right, lab, u.at[0, :, inner, :])
    pass_on = loads(stage_h, stage_lab, stage_u)
    keep_guess = pltpu.make_async_copy(guess.at[1 - xl, 0], guess_right, gr_sem)

    tables = [
        pltpu.make_async_copy(cond_hbm, cond_ref, load_sem.at[4]),
        pltpu.make_async_copy(cap_hbm, cap_ref, load_sem.at[5]),
    ]
    for copy in tables:
        copy.start()

    @pl.when(stays)
    def _():
        for copy in keep:
            copy.start()

    @pl.when(swapped)
    def _():
        for copy in pass_on:
            copy.start()

    @pl.when(jnp.logical_and(stays, takes_guess))
    def _():
        keep_guess.start()

    peers = 2 + 2 * ((xl + core) % 2) + jnp.where(has_left, 1, 0) + jnp.where(has_right, 1, 0)
    pl.semaphore_wait(barrier, peers)

    swap_h = [
        remote(stage_h.at[n], h_right.at[n], send_sem.at[n], h_sem.at[n], partner_id) for n in range(STEPS)
    ]
    swap_lab = remote(stage_lab, lab, send_sem.at[4], lab_sem, other_id)
    swap_u = remote(stage_u, u.at[0, :, inner, :], send_sem.at[5], u_sem.at[0], partner_id)
    swap_guess = remote(guess.at[xl, 0], guess_right, send_sem.at[6], gr_sem, partner_id)
    pass_guess = remote(guess_right, guess_left, send_sem.at[7], gl_sem, right_id)
    move_u = [
        remote(u.at[t, :, inner, :], u.at[t + 1, :, inner, :], send_sem.at[8 + t], u_sem.at[t + 1], down_id)
        for t in range(TICKS - 1)
    ]
    home_u = remote(u.at[TICKS - 1, :, inner, :], out_u.at[0], send_sem.at[8 + TICKS], out_sem.at[STEPS], home_id)

    def pass_h(n):
        return remote(h_right.at[n], h_left.at[n], hs_sem.at[n], hl_sem.at[n], right_id)

    sides = (left_id, right_id)

    def send_q(side, t, n):
        return remote(qs.at[side, t, n], qr.at[1 - side, t, n], qs_sem.at[t, side, n], q_sem.at[t, 1 - side, n], sides[side])

    def send_p(side, t, n):
        return remote(ps.at[side, t, n], pr.at[1 - side, t, n], ps_sem.at[t, side, n], p_sem.at[t, 1 - side, n], sides[side])

    def got_q(side, t, n):
        return remote(qs.at[side, t, n], qr.at[side, t, n], qs_sem.at[t, side, n], q_sem.at[t, side, n], left_id)

    def got_p(side, t, n):
        return remote(ps.at[side, t, n], pr.at[side, t, n], ps_sem.at[t, side, n], p_sem.at[t, side, n], left_id)

    def send_jump(t, n):
        return remote(jump_in.at[t, n], jump_far.at[t, n], in_sem.at[t, n], far_sem.at[t, n], outer_id)

    send_lab = remote(lab, lab_o, send_sem.at[8 + TICKS + 1], lab_o_sem, outer_id)

    def send_home(n):
        return remote(back.at[n], out_h.at[0, 0, n], bs_sem.at[n], out_sem.at[n], home_id)

    @pl.when(swapped)
    def _():
        pass_on[0].wait()
        swap_h[0].start()
        pass_on[1].wait()
        swap_lab.start()
        pass_on[2].wait()
        swap_u.start()
        pass_on[3].wait()
        for copy in swap_h[1:]:
            copy.start()

    @pl.when(jnp.logical_and(swapped, takes_guess))
    def _():
        swap_guess.start()

    @pl.when(stays)
    def _():
        keep[0].wait()

    pl.when(swapped)(swap_h[0].wait_recv)
    pl.when(has_right)(pass_h(0).start)

    @pl.when(stays)
    def _():
        keep[3].wait()
        for n in range(1, STEPS):
            pl.when(has_right)(pass_h(n).start)

        @pl.when(takes_guess)
        def _():
            keep_guess.wait()
            pl.when(has_right)(pass_guess.start)

    nothing = jnp.zeros((NY, NZ), F32)

    @pl.when(jnp.logical_not(has_right))
    def _():
        h_right[0] = nothing
        pl.when(stays)(lambda: h_right.__setitem__(slice(1, STEPS), jnp.zeros((STEPS - 1, NY, NZ), F32)))

    @pl.when(jnp.logical_not(has_left))
    def _():
        h_left[...] = jnp.zeros((STEPS, NY, NZ), F32)

    def pass_rest(n):
        @pl.when(jnp.logical_and(swapped, n == 0))
        def _():
            for follow in range(1, STEPS):
                swap_h[follow].wait_recv()
                pl.when(has_right)(pass_h(follow).start)

            @pl.when(jnp.logical_not(has_right))
            def _():
                h_right[1:STEPS] = jnp.zeros((STEPS - 1, NY, NZ), F32)

    pl.when(stays)(keep[1].wait)
    pl.when(swapped)(swap_lab.wait_recv)

    for copy in tables:
        copy.wait()

    def pick(table, value):
        result = jnp.full(value.shape, table[0], F32)
        for cls in range(1, 4):
            result = jnp.where(value == cls, table[cls], result)
        return result

    pl.when(long)(send_lab.start)
    lane = lax.broadcasted_iota(jnp.int32, (CHUNK, NZ), 1)
    line = lax.broadcasted_iota(jnp.int32, (CHUNK, NZ), 0)

    def coefficients(label, scratch, edges, own):
        for plane in range(2):
            for row in range(0, NY, CHUNK):
                scratch[plane, PAD + row : PAD + row + CHUNK, :] = pick(cond_ref, label[plane, row : row + CHUNK, :])
        for plane in range(2):
            for row in range(0, NY, CHUNK):
                here = slice(row, row + CHUNK)
                base = PAD + row
                k = scratch[plane, base : base + CHUNK, :]
                twice = 2.0 * k
                face_x = harmonic(k, scratch[1 - plane, base : base + CHUNK, :])
                face_u = harmonic(k, scratch[plane, base - 1 : base - 1 + CHUNK, :])
                face_d = harmonic(k, scratch[plane, base + 1 : base + 1 + CHUNK, :])
                face_l = jnp.where(lane == 0, 0.0, harmonic(k, pltpu.roll(k, 1, 1)))
                face_r = jnp.where(lane == NZ - 1, 0.0, harmonic(k, pltpu.roll(k, NZ - 1, 1)))
                side_u = jnp.where(line + row == 0, twice, face_u) if row == 0 else face_u
                side_d = jnp.where(line + row == NY - 1, twice, face_d) if row + CHUNK == NY else face_d
                side_l = jnp.where(lane == 0, twice, face_l)
                side_r = jnp.where(lane == NZ - 1, twice, face_r)
                capacity = pick(cap_ref, label[plane, here, :])
                common = capacity + face_x + side_u + side_d + side_l + side_r
                faces = (face_x, face_u, face_d, face_l, face_r, capacity)
                if own:
                    inv_neu = 1.0 / jnp.where(edges[plane], common, common + twice)
                    inv_dir = 1.0 / (common + twice)
                    for j, face in enumerate(faces):
                        co_d[j, plane, here, :] = face * inv_dir
                    co_d[6, plane, here, :] = twice * inv_dir
                    end[plane, here, :] = twice
                else:
                    inv_neu = 1.0 / common
                for j, face in enumerate(faces):
                    (co_n if own else co_o)[j, plane, here, :] = face * inv_neu
                (inv_n if own else inv_o)[plane, here, :] = inv_neu

    coefficients(lab, buf_a, exists, True)

    pl.when(stays)(keep[2].wait)
    pl.when(swapped)(swap_u.wait_recv)

    last = TICKS - 1

    def inner_jump(t, n, carry):
        got_q(1 - core, t, n).wait_recv()
        for row in range(0, NY, CHUNK):
            here = slice(row, row + CHUNK)
            jump_in[t, n, here, :] = qs[1 - core, t, n, here, :] + qr[1 - core, t, n, here, :]
        if t < last:
            send_jump(t, n).start()
        else:
            pl.when(outer_left)(send_jump(t, n).start)
        return carry

    def outer(t, n):
        send_jump(t, n).wait_recv()
        near, far = 1 - core, core
        for row in range(0, NY, CHUNK):
            here = slice(row, row + CHUNK)
            rows = slice(PAD + row, PAD + row + CHUNK)
            jump = qs[core, t, n, here, :] + qr[core, t, n, here, :]
            rhs[near, here, :] = inv_o[near, here, :] * jump + co_o[5, near, here, :] * psi_o[near, rows, :]
            rhs[far, here, :] = (
                inv_o[far, here, :] * jump_far[t, n, here, :] + co_o[5, far, here, :] * psi_o[far, rows, :]
            )
        sweep(psi_o, buf_a, rhs, co_o)
        sweep(buf_a, buf_b, rhs, co_o)
        sweep(buf_b, psi_o, rhs, co_o)
        for row in range(0, NY, CHUNK):
            pr[core, t, n, row : row + CHUNK, :] = psi_o[near, PAD + row : PAD + row + CHUNK, :]

    for tick in range(TICKS):
        state = u.at[tick]
        if tick > 0:
            move_u[tick - 1].wait_recv()
            pl.when(jnp.logical_and(restart[tick], has_left))(pass_guess.wait_recv)

        def dirichlet(n, carry, tick=tick, state=state):
            if tick == 0:
                pl.when(has_left)(pass_h(n).wait_recv)
            else:
                if tick == 1:
                    pl.when(has_right)(pass_h(n).wait_send)

                @pl.when(useful[tick - 1])
                def _():
                    pl.when(long)(lambda: outer(tick - 1, n))
                    for side, trace in enumerate((h_left, h_right)):
                        pl.when(p_uses[side])(got_p(side, tick - 1, n).wait_recv)
                        for row in range(0, NY, CHUNK):
                            here = slice(row, row + CHUNK)
                            both = ps[side, tick - 1, n, here, :] + pr[side, tick - 1, n, here, :]
                            new = trace[n, here, :] + 0.25 * both
                            trace[n, here, :] = jnp.where(exists[side], new, 0.0)

                @pl.when(restart[tick])
                def _():
                    for side, (trace, taken) in enumerate(((h_left, guess_left), (h_right, guess_right))):
                        for row in range(0, NY, CHUNK):
                            here = slice(row, row + CHUNK)
                            trace[n, here, :] = jnp.where(exists[side], taken[n, here, :], 0.0)

            for plane, trace in enumerate((h_left, h_right)):
                for row in range(0, NY, CHUNK):
                    here = slice(row, row + CHUNK)
                    rhs[plane, here, :] = (
                        co_d[5, plane, here, :] * state[plane, PAD + row : PAD + row + CHUNK, :]
                        + co_d[6, plane, here, :] * trace[n, here, :]
                    )

            def flux(plane, here, value):
                trace = (h_left, h_right)[plane]
                qs[plane, tick, n, here, :] = end[plane, here, :] * (value - trace[n, here, :])

            sweep(state, buf_a, rhs, co_d)
            sweep(buf_a, buf_b, rhs, co_d)
            sweep(buf_b, state, rhs, co_d, flux)
            pl.when(jnp.logical_and(has_right, useful[tick]))(send_q(1, tick, n).start)
            pl.when(jnp.logical_and(has_left, useful[tick]))(send_q(0, tick, n).start)
            if tick == 0:
                pass_rest(n)
            return carry

        lax.fori_loop(0, STEPS, dirichlet, 0)
        if tick + 1 < TICKS:
            move_u[tick].start()
        else:
            home_u.start()
        if tick + 1 < TICKS:

            @pl.when(jnp.logical_and(swapped, restart[tick + 1]))
            def _():
                swap_guess.wait_recv()
                pl.when(has_right)(pass_guess.start)

        if tick == 0:

            @pl.when(long)
            def _():
                send_lab.wait_recv()
                coefficients(lab_o, psi_o, None, False)

        @pl.when(jnp.logical_and(long, useful[tick]))
        def _():
            lax.fori_loop(0, STEPS, functools.partial(inner_jump, tick), 0)
            psi_o[:, PAD : PAD + NY, :] = jnp.zeros((2, NY, NZ), F32)

        def neumann(n, carry, tick=tick, first=False):
            for side in range(2):
                pl.when(q_wait[side])(got_q(side, tick, n).wait_recv)
            for plane in range(2):
                for row in range(0, NY, CHUNK):
                    here = slice(row, row + CHUNK)
                    jump = qs[plane, tick, n, here, :] + qr[plane, tick, n, here, :]
                    value = inv_n[plane, here, :] * jnp.where(exists[plane], jump, 0.0)
                    if not first:
                        value = value + co_n[5, plane, here, :] * psi[plane, PAD + row : PAD + row + CHUNK, :]
                    rhs[plane, here, :] = value
                    if first:
                        buf_a[plane, PAD + row : PAD + row + CHUNK, :] = value

            def ends(plane, here, value):
                ps[plane, tick, n, here, :] = value

            if not first:
                sweep(psi, buf_a, rhs, co_n)
            sweep(buf_a, buf_b, rhs, co_n)
            sweep(buf_b, psi, rhs, co_n, ends)
            pl.when(p_uses[0])(send_p(0, tick, n).start)
            if tick + 1 < TICKS:
                pl.when(p_uses[1])(send_p(1, tick, n).start)
            return carry

        @pl.when(useful[tick])
        def _():
            neumann(0, 0, first=True)
            lax.fori_loop(1, STEPS, neumann, 0)


    def finish(n, carry):
        pl.when(outer_right)(lambda: outer(last, n))
        pl.when(p_uses[1])(got_p(1, last, n).wait_recv)
        for row in range(0, NY, CHUNK):
            here = slice(row, row + CHUNK)
            new = h_right[n, here, :] + 0.25 * (ps[1, last, n, here, :] + pr[1, last, n, here, :])
            back[n, here, :] = jnp.where(has_right, new, 0.0)
        send_home(n).start()
        return carry

    lax.fori_loop(0, STEPS, finish, 0)

    @pl.when(swapped)
    def _():
        for copy in swap_h:
            copy.wait_send()
        swap_lab.wait_send()
        swap_u.wait_send()

    pl.when(jnp.logical_and(swapped, takes_guess))(swap_guess.wait_send)
    pl.when(jnp.logical_and(takes_guess, has_right))(pass_guess.wait_send)
    for copy in move_u:
        copy.wait_send()
    home_u.wait_send()

    for side in range(2):

        @pl.when(exists[side])
        def _():
            for n in range(STEPS):
                for t in range(TICKS):
                    pl.when(useful[t])(send_q(side, t, n).wait_send)

        @pl.when(p_uses[side])
        def _():
            for n in range(STEPS):
                for t in range(TICKS if side == 0 else last):
                    pl.when(useful[t])(send_p(side, t, n).wait_send)

    @pl.when(long)
    def _():
        send_lab.wait_send()
        for n in range(STEPS):
            for t in range(last):
                pl.when(useful[t])(send_jump(t, n).wait_send)

    @pl.when(outer_left)
    def _():
        for n in range(STEPS):
            send_jump(last, n).wait_send()

    for n in range(STEPS):
        send_home(n).wait_send()
    home_u.wait_recv()
    for n in range(STEPS):
        send_home(n).wait_recv()


def deliver(field, trace, out_field, out_trace, block, in_sem, out_sem):
    pieces = [(field.at[0, i], out_field.at[0, i]) for i in range(2)]
    pieces += [(trace.at[0, 0, n], out_trace.at[0, 0, n]) for n in range(STEPS)]
    loads = [pltpu.make_async_copy(src, block.at[i], in_sem.at[i]) for i, (src, _) in enumerate(pieces)]
    stores = [pltpu.make_async_copy(block.at[i], dst, out_sem.at[i]) for i, (_, dst) in enumerate(pieces)]
    for copy in loads:
        copy.start()
    for load, store in zip(loads, stores):
        load.wait()
        store.start()
    for store in stores:
        store.wait()


def local(fields, labels, traces, new_guess, cond_table, cap_table):
    plane = (NY, NZ)
    field = (2, ROWS, NZ)
    vm = lambda *shape: pltpu.VMEM(shape, F32)
    dma = lambda *shape: pltpu.SemaphoreType.DMA(shape)
    any_spec = pl.BlockSpec(memory_space=pl.ANY)
    hbm = pl.BlockSpec(memory_space=pltpu.HBM)
    per_step = (TICKS, STEPS) + plane
    results = pl.pallas_call(
        kernel,
        out_shape=(
            jax.ShapeDtypeStruct((1, 2) + plane, F32),
            jax.ShapeDtypeStruct((1, 1, STEPS) + plane, F32),
        ),
        in_specs=[hbm] * 6,
        out_specs=(any_spec, any_spec),
        scratch_shapes=[
            pltpu.SMEM((4,), F32),
            pltpu.SMEM((4,), F32),
            pltpu.VMEM((2,) + plane, jnp.int32),
            vm(2, *plane),
            vm(STEPS, *plane),
            pltpu.VMEM((2,) + plane, jnp.int32),
            vm(TICKS, *field),
            vm(STEPS, *plane),
            vm(STEPS, *plane),
            vm(STEPS, *plane),
            vm(STEPS, *plane),
            vm(*field),
            vm(*field),
            vm(*field),
            vm(2, *plane),
            vm(7, 2, *plane),
            vm(6, 2, *plane),
            vm(2, *plane),
            vm(2, *plane),
            vm(2, *per_step),
            vm(2, *per_step),
            vm(2, *per_step),
            vm(2, *per_step),
            vm(STEPS, *plane),
            pltpu.VMEM((2,) + plane, jnp.int32),
            vm(6, 2, *plane),
            vm(2, *plane),
            vm(*field),
            vm(*per_step),
            vm(*per_step),
            pltpu.SemaphoreType.DMA,
            dma(TICKS),
            dma(STEPS),
            dma(STEPS),
            pltpu.SemaphoreType.DMA,
            pltpu.SemaphoreType.DMA,
            dma(TICKS, 2, STEPS),
            dma(TICKS, 2, STEPS),
            dma(STEPS + 1),
            dma(6),
            dma(8 + TICKS + 2),
            dma(TICKS, 2, STEPS),
            dma(TICKS, 2, STEPS),
            dma(STEPS),
            dma(STEPS),
            pltpu.SemaphoreType.DMA,
            dma(TICKS, STEPS),
            dma(TICKS, STEPS),
        ],
        compiler_params=pltpu.CompilerParams(collective_id=0, has_side_effects=True),
    )(cond_table, cap_table, fields, labels, traces, new_guess)
    return pl.pallas_call(
        deliver,
        out_shape=(
            jax.ShapeDtypeStruct((1, 2) + plane, F32),
            jax.ShapeDtypeStruct((1, 1, STEPS) + plane, F32),
        ),
        in_specs=[any_spec] * 2,
        out_specs=(any_spec, any_spec),
        scratch_shapes=[vm(2 + STEPS, *plane), dma(2 + STEPS), dma(2 + STEPS)],
    )(*results)


def solution(mesh):
    return jax.shard_map(
        local,
        mesh=mesh,
        in_specs=(
            P("iter", "sub", None, None),
            P("sub", None, None),
            P("iter", "sub", None, None, None),
            P(None, "sub", None, None, None),
            P(),
            P(),
        ),
        out_specs=(P("iter", "sub", None, None), P("iter", "sub", None, None, None)),
        check_vma=False,
    )
```

```python
import functools

import jax
import jax.numpy as jnp
from jax import lax
from jax.experimental import pallas as pl
from jax.experimental.pallas import tpu as pltpu
from jax.sharding import PartitionSpec as P

MESH = pl.DeviceIdType.MESH
TICKS = 3
STEPS = 4
NY = 128
NZ = 128
PAD = 8
ROWS = NY + 2 * PAD
CHUNK = 32
SPAN = 8
F32 = jnp.float32


def harmonic(first, second):
    return 2.0 * first * second / (first + second)


def sweep(source, target, rhs, coeff, extra=None):
    for plane in range(2):
        for row in range(0, NY, CHUNK):
            here = slice(row, row + CHUNK)
            base = PAD + row
            v = source[plane, base : base + CHUNK, :]
            out = rhs[plane, here, :]
            out = out + coeff[0, plane, here, :] * source[1 - plane, base : base + CHUNK, :]
            out = out + coeff[1, plane, here, :] * source[plane, base - 1 : base - 1 + CHUNK, :]
            out = out + coeff[2, plane, here, :] * source[plane, base + 1 : base + 1 + CHUNK, :]
            out = out + coeff[3, plane, here, :] * pltpu.roll(v, 1, 1)
            out = out + coeff[4, plane, here, :] * pltpu.roll(v, NZ - 1, 1)
            target[plane, base : base + CHUNK, :] = out
            if extra is not None:
                extra(plane, here, out)


def kernel(
    cond_hbm, cap_hbm, fields, labels, traces, guess,
    out_u, out_h,
    cond_ref, cap_ref,
    stage_lab, stage_u, stage_h, lab, u, h_right, h_left, guess_right, guess_left,
    psi, buf_a, buf_b, rhs, co_d, co_n, end, inv_n,
    qs, qr, ps, pr, back,
    lab_o, co_o, inv_o, psi_o, jump_in, jump_far,
    lab_sem, u_sem, h_sem, hl_sem, gr_sem, gl_sem,
    q_sem, p_sem, out_sem, load_sem, send_sem, qs_sem, ps_sem, hs_sem, bs_sem,
    lab_o_sem, far_sem, in_sem,
):
    sub = lax.axis_index("sub")
    it = lax.axis_index("iter")
    pair = sub // 2
    xl = sub % 2
    xh = it // 2
    core = it % 2
    ring = 2 * xh + xl
    slab = 2 * pair + core
    pairs = lax.axis_size("sub") // 2
    has_left = slab > 0
    has_right = slab < 2 * pairs - 1
    swapped = xl != core
    stays = xl == core
    takes_guess = xh == 1

    outer_right = jnp.logical_and(jnp.logical_and(core == 1, has_right), pair % SPAN == SPAN - 1)
    outer_left = jnp.logical_and(jnp.logical_and(core == 0, has_left), pair % SPAN == 0)
    long = jnp.logical_or(outer_right, outer_left)
    short = jnp.logical_not(long)
    exists = (has_left, has_right)
    restart = [None] + [ring == 4 - tick for tick in range(1, TICKS)]
    useful = [ring != 3 - tick for tick in range(TICKS - 1)] + [ring >= 0]
    q_wait = (
        jnp.logical_and(has_left, jnp.logical_not(outer_right)),
        jnp.logical_and(has_right, jnp.logical_not(outer_left)),
    )
    p_uses = (
        jnp.logical_and(has_left, jnp.logical_not(outer_left)),
        jnp.logical_and(has_right, jnp.logical_not(outer_right)),
    )
    outer_id = {"sub": sub + 4 * core - 2, "iter": it + 1 - 2 * core}

    right_id = {"sub": sub + 2 * core, "iter": it + 1 - 2 * core}
    left_id = {"sub": sub - 2 * (1 - core), "iter": it + 1 - 2 * core}
    partner_id = {"sub": sub + 1 - 2 * xl, "iter": it + 1 - 2 * core}
    down = (ring + 3) % 4
    up = (ring + 1) % 4
    down_id = {"sub": 2 * pair + down % 2, "iter": 2 * (down // 2) + core}
    up_id = {"sub": 2 * pair + up % 2, "iter": 2 * (up // 2) + core}
    other = (ring + 1 + 2 * core) % 4
    other_id = {"sub": 2 * pair + other % 2, "iter": 2 * (other // 2) + 1 - core}
    home_id = {"sub": 2 * pair + core, "iter": (ring + 2) % 4}
    source_ring = (it + 2) % 4
    source_id = {"sub": 2 * pair + source_ring % 2, "iter": 2 * (source_ring // 2) + xl}

    def remote(src, dst, send, recv, device):
        return pltpu.make_async_remote_copy(
            src_ref=src, dst_ref=dst, send_sem=send, recv_sem=recv, device_id=device, device_id_type=MESH
        )

    inner = pl.ds(PAD, NY)

    zero_pad = jnp.zeros((2, PAD, NZ), F32)
    for ref in (buf_a, buf_b, psi, psi_o):
        ref[:, 0:PAD, :] = zero_pad
        ref[:, PAD + NY : ROWS, :] = zero_pad
    for tick in range(TICKS):
        u[tick, :, 0:PAD, :] = zero_pad
        u[tick, :, PAD + NY : ROWS, :] = zero_pad

    barrier = pltpu.get_barrier_semaphore()

    def greet(device):
        pl.semaphore_signal(barrier, inc=1, device_id=device, device_id_type=MESH)

    pl.when(has_left)(lambda: greet(left_id))
    pl.when(has_right)(lambda: greet(right_id))
    pl.when(swapped)(lambda: greet(partner_id))
    pl.when(swapped)(lambda: greet(other_id))
    greet(up_id)
    greet(source_id)

    def loads(d_h, d_lab, d_u):
        return [
            pltpu.make_async_copy(traces.at[0, 0, 0:1], d_h.at[0:1], load_sem.at[0]),
            pltpu.make_async_copy(labels, d_lab, load_sem.at[1]),
            pltpu.make_async_copy(fields.at[0], d_u, load_sem.at[2]),
            pltpu.make_async_copy(traces.at[0, 0, 1:STEPS], d_h.at[1:STEPS], load_sem.at[3]),
        ]

    keep = loads(h_right, lab, u.at[0, :, inner, :])
    pass_on = loads(stage_h, stage_lab, stage_u)
    keep_guess = pltpu.make_async_copy(guess.at[1 - xl, 0], guess_right, gr_sem)

    tables = [
        pltpu.make_async_copy(cond_hbm, cond_ref, load_sem.at[4]),
        pltpu.make_async_copy(cap_hbm, cap_ref, load_sem.at[5]),
    ]
    for copy in tables:
        copy.start()

    @pl.when(stays)
    def _():
        for copy in keep:
            copy.start()

    @pl.when(swapped)
    def _():
        for copy in pass_on:
            copy.start()

    @pl.when(jnp.logical_and(stays, takes_guess))
    def _():
        keep_guess.start()

    peers = 2 + 2 * ((xl + core) % 2) + jnp.where(has_left, 1, 0) + jnp.where(has_right, 1, 0)
    pl.semaphore_wait(barrier, peers)

    swap_h = [
        remote(stage_h.at[n], h_right.at[n], send_sem.at[n], h_sem.at[n], partner_id) for n in range(STEPS)
    ]
    swap_lab = remote(stage_lab, lab, send_sem.at[4], lab_sem, other_id)
    swap_u = remote(stage_u, u.at[0, :, inner, :], send_sem.at[5], u_sem.at[0], partner_id)
    swap_guess = remote(guess.at[xl, 0], guess_right, send_sem.at[6], gr_sem, partner_id)
    pass_guess = remote(guess_right, guess_left, send_sem.at[7], gl_sem, right_id)
    move_u = [
        remote(u.at[t, :, inner, :], u.at[t + 1, :, inner, :], send_sem.at[8 + t], u_sem.at[t + 1], down_id)
        for t in range(TICKS - 1)
    ]
    home_u = remote(u.at[TICKS - 1, :, inner, :], out_u.at[0], send_sem.at[8 + TICKS], out_sem.at[STEPS], home_id)

    def pass_h(n):
        return remote(h_right.at[n], h_left.at[n], hs_sem.at[n], hl_sem.at[n], right_id)

    sides = (left_id, right_id)

    def send_q(side, t, n):
        return remote(qs.at[side, t, n], qr.at[1 - side, t, n], qs_sem.at[t, side, n], q_sem.at[t, 1 - side, n], sides[side])

    def send_p(side, t, n):
        return remote(ps.at[side, t, n], pr.at[1 - side, t, n], ps_sem.at[t, side, n], p_sem.at[t, 1 - side, n], sides[side])

    def got_q(side, t, n):
        return remote(qs.at[side, t, n], qr.at[side, t, n], qs_sem.at[t, side, n], q_sem.at[t, side, n], left_id)

    def got_p(side, t, n):
        return remote(ps.at[side, t, n], pr.at[side, t, n], ps_sem.at[t, side, n], p_sem.at[t, side, n], left_id)

    def send_jump(t, n):
        return remote(jump_in.at[t, n], jump_far.at[t, n], in_sem.at[t, n], far_sem.at[t, n], outer_id)

    send_lab = remote(lab, lab_o, send_sem.at[8 + TICKS + 1], lab_o_sem, outer_id)

    def send_home(n):
        return remote(back.at[n], out_h.at[0, 0, n], bs_sem.at[n], out_sem.at[n], home_id)

    @pl.when(swapped)
    def _():
        pass_on[0].wait()
        swap_h[0].start()
        pass_on[1].wait()
        swap_lab.start()
        pass_on[3].wait()
        for copy in swap_h[1:]:
            copy.start()
        pass_on[2].wait()
        swap_u.start()

    @pl.when(jnp.logical_and(swapped, takes_guess))
    def _():
        swap_guess.start()

    @pl.when(stays)
    def _():
        keep[0].wait()
        keep[3].wait()

    for n in range(STEPS):
        pl.when(swapped)(swap_h[n].wait_recv)
        pl.when(has_right)(pass_h(n).start)

    @pl.when(jnp.logical_and(stays, takes_guess))
    def _():
        keep_guess.wait()
        pl.when(has_right)(pass_guess.start)

    @pl.when(jnp.logical_not(has_right))
    def _():
        h_right[...] = jnp.zeros((STEPS, NY, NZ), F32)

    @pl.when(jnp.logical_not(has_left))
    def _():
        h_left[...] = jnp.zeros((STEPS, NY, NZ), F32)

    pl.when(stays)(keep[1].wait)
    pl.when(swapped)(swap_lab.wait_recv)

    for copy in tables:
        copy.wait()

    def pick(table, value):
        result = jnp.full(value.shape, table[0], F32)
        for cls in range(1, 4):
            result = jnp.where(value == cls, table[cls], result)
        return result

    pl.when(long)(send_lab.start)
    lane = lax.broadcasted_iota(jnp.int32, (CHUNK, NZ), 1)
    line = lax.broadcasted_iota(jnp.int32, (CHUNK, NZ), 0)

    def coefficients(label, scratch, edges, own):
        for plane in range(2):
            for row in range(0, NY, CHUNK):
                scratch[plane, PAD + row : PAD + row + CHUNK, :] = pick(cond_ref, label[plane, row : row + CHUNK, :])
        for plane in range(2):
            for row in range(0, NY, CHUNK):
                here = slice(row, row + CHUNK)
                base = PAD + row
                k = scratch[plane, base : base + CHUNK, :]
                twice = 2.0 * k
                face_x = harmonic(k, scratch[1 - plane, base : base + CHUNK, :])
                face_u = harmonic(k, scratch[plane, base - 1 : base - 1 + CHUNK, :])
                face_d = harmonic(k, scratch[plane, base + 1 : base + 1 + CHUNK, :])
                face_l = jnp.where(lane == 0, 0.0, harmonic(k, pltpu.roll(k, 1, 1)))
                face_r = jnp.where(lane == NZ - 1, 0.0, harmonic(k, pltpu.roll(k, NZ - 1, 1)))
                side_u = jnp.where(line + row == 0, twice, face_u) if row == 0 else face_u
                side_d = jnp.where(line + row == NY - 1, twice, face_d) if row + CHUNK == NY else face_d
                side_l = jnp.where(lane == 0, twice, face_l)
                side_r = jnp.where(lane == NZ - 1, twice, face_r)
                capacity = pick(cap_ref, label[plane, here, :])
                common = capacity + face_x + side_u + side_d + side_l + side_r
                faces = (face_x, face_u, face_d, face_l, face_r, capacity)
                if own:
                    inv_neu = 1.0 / jnp.where(edges[plane], common, common + twice)
                    inv_dir = 1.0 / (common + twice)
                    for j, face in enumerate(faces):
                        co_d[j, plane, here, :] = face * inv_dir
                    co_d[6, plane, here, :] = twice * inv_dir
                    end[plane, here, :] = twice
                else:
                    inv_neu = 1.0 / common
                for j, face in enumerate(faces):
                    (co_n if own else co_o)[j, plane, here, :] = face * inv_neu
                (inv_n if own else inv_o)[plane, here, :] = inv_neu

    coefficients(lab, buf_a, exists, True)

    pl.when(stays)(keep[2].wait)
    pl.when(swapped)(swap_u.wait_recv)

    last = TICKS - 1

    def inner_jump(t, n, carry):
        got_q(1 - core, t, n).wait_recv()
        for row in range(0, NY, CHUNK):
            here = slice(row, row + CHUNK)
            jump_in[t, n, here, :] = qs[1 - core, t, n, here, :] + qr[1 - core, t, n, here, :]
        if t < last:
            send_jump(t, n).start()
        else:
            pl.when(outer_left)(send_jump(t, n).start)
        return carry

    def outer(t, n):
        send_jump(t, n).wait_recv()
        near, far = 1 - core, core
        for row in range(0, NY, CHUNK):
            here = slice(row, row + CHUNK)
            rows = slice(PAD + row, PAD + row + CHUNK)
            jump = qs[core, t, n, here, :] + qr[core, t, n, here, :]
            rhs[near, here, :] = inv_o[near, here, :] * jump + co_o[5, near, here, :] * psi_o[near, rows, :]
            rhs[far, here, :] = (
                inv_o[far, here, :] * jump_far[t, n, here, :] + co_o[5, far, here, :] * psi_o[far, rows, :]
            )
        sweep(psi_o, buf_a, rhs, co_o)
        sweep(buf_a, buf_b, rhs, co_o)
        sweep(buf_b, psi_o, rhs, co_o)
        for row in range(0, NY, CHUNK):
            pr[core, t, n, row : row + CHUNK, :] = psi_o[near, PAD + row : PAD + row + CHUNK, :]

    for tick in range(TICKS):
        state = u.at[tick]
        if tick > 0:
            pl.when(jnp.logical_and(restart[tick], has_left))(pass_guess.wait_recv)

        def dirichlet(n, carry, tick=tick, state=state):
            if tick == 0:
                pl.when(has_left)(pass_h(n).wait_recv)
            else:
                if tick == 1:
                    pl.when(has_right)(pass_h(n).wait_send)

                @pl.when(useful[tick - 1])
                def _():
                    pl.when(long)(lambda: outer(tick - 1, n))
                    for side, trace in enumerate((h_left, h_right)):
                        pl.when(p_uses[side])(got_p(side, tick - 1, n).wait_recv)
                        for row in range(0, NY, CHUNK):
                            here = slice(row, row + CHUNK)
                            both = ps[side, tick - 1, n, here, :] + pr[side, tick - 1, n, here, :]
                            new = trace[n, here, :] + 0.25 * both
                            trace[n, here, :] = jnp.where(exists[side], new, 0.0)

                @pl.when(restart[tick])
                def _():
                    for side, (trace, taken) in enumerate(((h_left, guess_left), (h_right, guess_right))):
                        for row in range(0, NY, CHUNK):
                            here = slice(row, row + CHUNK)
                            trace[n, here, :] = jnp.where(exists[side], taken[n, here, :], 0.0)

                pl.when(n == 0)(move_u[tick - 1].wait_recv)

            for plane, trace in enumerate((h_left, h_right)):
                for row in range(0, NY, CHUNK):
                    here = slice(row, row + CHUNK)
                    rhs[plane, here, :] = (
                        co_d[5, plane, here, :] * state[plane, PAD + row : PAD + row + CHUNK, :]
                        + co_d[6, plane, here, :] * trace[n, here, :]
                    )

            def flux(plane, here, value):
                trace = (h_left, h_right)[plane]
                qs[plane, tick, n, here, :] = end[plane, here, :] * (value - trace[n, here, :])

            sweep(state, buf_a, rhs, co_d)
            sweep(buf_a, buf_b, rhs, co_d)
            sweep(buf_b, state, rhs, co_d, flux)
            pl.when(jnp.logical_and(has_right, useful[tick]))(send_q(1, tick, n).start)
            pl.when(jnp.logical_and(has_left, useful[tick]))(send_q(0, tick, n).start)
            return carry

        lax.fori_loop(0, STEPS, dirichlet, 0)
        if tick + 1 < TICKS:
            move_u[tick].start()
        else:
            home_u.start()
        if tick + 1 < TICKS:

            @pl.when(jnp.logical_and(swapped, restart[tick + 1]))
            def _():
                swap_guess.wait_recv()
                pl.when(has_right)(pass_guess.start)

        @pl.when(jnp.logical_and(long, useful[tick]))
        def _():
            lax.fori_loop(0, STEPS, functools.partial(inner_jump, tick), 0)

        def neumann(n, carry, tick=tick, first=False):
            for side in range(2):
                pl.when(q_wait[side])(got_q(side, tick, n).wait_recv)
            for plane in range(2):
                for row in range(0, NY, CHUNK):
                    here = slice(row, row + CHUNK)
                    jump = qs[plane, tick, n, here, :] + qr[plane, tick, n, here, :]
                    value = inv_n[plane, here, :] * jnp.where(exists[plane], jump, 0.0)
                    if not first:
                        value = value + co_n[5, plane, here, :] * psi[plane, PAD + row : PAD + row + CHUNK, :]
                    rhs[plane, here, :] = value
                    if first:
                        buf_a[plane, PAD + row : PAD + row + CHUNK, :] = value

            def ends(plane, here, value):
                ps[plane, tick, n, here, :] = value

            if not first:
                sweep(psi, buf_a, rhs, co_n)
            sweep(buf_a, buf_b, rhs, co_n)
            sweep(buf_b, psi, rhs, co_n, ends)
            pl.when(p_uses[0])(send_p(0, tick, n).start)
            if tick + 1 < TICKS:
                pl.when(p_uses[1])(send_p(1, tick, n).start)
            return carry

        @pl.when(useful[tick])
        def _():
            neumann(0, 0, first=True)

        @pl.when(long)
        def _():
            if tick == 0:
                send_lab.wait_recv()
                coefficients(lab_o, psi_o, None, False)
            psi_o[:, PAD : PAD + NY, :] = jnp.zeros((2, NY, NZ), F32)

        @pl.when(useful[tick])
        def _():
            lax.fori_loop(1, STEPS, neumann, 0)


    def finish(n, carry):
        pl.when(outer_right)(lambda: outer(last, n))
        pl.when(p_uses[1])(got_p(1, last, n).wait_recv)
        for row in range(0, NY, CHUNK):
            here = slice(row, row + CHUNK)
            new = h_right[n, here, :] + 0.25 * (ps[1, last, n, here, :] + pr[1, last, n, here, :])
            back[n, here, :] = jnp.where(has_right, new, 0.0)
        send_home(n).start()
        return carry

    lax.fori_loop(0, STEPS, finish, 0)

    @pl.when(swapped)
    def _():
        for copy in swap_h:
            copy.wait_send()
        swap_lab.wait_send()
        swap_u.wait_send()

    pl.when(jnp.logical_and(swapped, takes_guess))(swap_guess.wait_send)
    pl.when(jnp.logical_and(takes_guess, has_right))(pass_guess.wait_send)
    for copy in move_u:
        copy.wait_send()
    home_u.wait_send()

    for side in range(2):

        @pl.when(exists[side])
        def _():
            for n in range(STEPS):
                for t in range(TICKS):
                    pl.when(useful[t])(send_q(side, t, n).wait_send)

        @pl.when(p_uses[side])
        def _():
            for n in range(STEPS):
                for t in range(TICKS if side == 0 else last):
                    pl.when(useful[t])(send_p(side, t, n).wait_send)

    @pl.when(long)
    def _():
        send_lab.wait_send()
        for n in range(STEPS):
            for t in range(last):
                pl.when(useful[t])(send_jump(t, n).wait_send)

    @pl.when(outer_left)
    def _():
        for n in range(STEPS):
            send_jump(last, n).wait_send()

    for n in range(STEPS):
        send_home(n).wait_send()
    home_u.wait_recv()
    for n in range(STEPS):
        send_home(n).wait_recv()


def deliver(field, trace, out_field, out_trace, block, in_sem, out_sem):
    pieces = [(field.at[0, i], out_field.at[0, i]) for i in range(2)]
    pieces += [(trace.at[0, 0, n], out_trace.at[0, 0, n]) for n in range(STEPS)]
    loads = [pltpu.make_async_copy(src, block.at[i], in_sem.at[i]) for i, (src, _) in enumerate(pieces)]
    stores = [pltpu.make_async_copy(block.at[i], dst, out_sem.at[i]) for i, (_, dst) in enumerate(pieces)]
    for copy in loads:
        copy.start()
    for load, store in zip(loads, stores):
        load.wait()
        store.start()
    for store in stores:
        store.wait()


def local(fields, labels, traces, new_guess, cond_table, cap_table):
    plane = (NY, NZ)
    field = (2, ROWS, NZ)
    vm = lambda *shape: pltpu.VMEM(shape, F32)
    dma = lambda *shape: pltpu.SemaphoreType.DMA(shape)
    any_spec = pl.BlockSpec(memory_space=pl.ANY)
    hbm = pl.BlockSpec(memory_space=pltpu.HBM)
    per_step = (TICKS, STEPS) + plane
    results = pl.pallas_call(
        kernel,
        out_shape=(
            jax.ShapeDtypeStruct((1, 2) + plane, F32),
            jax.ShapeDtypeStruct((1, 1, STEPS) + plane, F32),
        ),
        in_specs=[hbm] * 6,
        out_specs=(any_spec, any_spec),
        scratch_shapes=[
            pltpu.SMEM((4,), F32),
            pltpu.SMEM((4,), F32),
            pltpu.VMEM((2,) + plane, jnp.int32),
            vm(2, *plane),
            vm(STEPS, *plane),
            pltpu.VMEM((2,) + plane, jnp.int32),
            vm(TICKS, *field),
            vm(STEPS, *plane),
            vm(STEPS, *plane),
            vm(STEPS, *plane),
            vm(STEPS, *plane),
            vm(*field),
            vm(*field),
            vm(*field),
            vm(2, *plane),
            vm(7, 2, *plane),
            vm(6, 2, *plane),
            vm(2, *plane),
            vm(2, *plane),
            vm(2, *per_step),
            vm(2, *per_step),
            vm(2, *per_step),
            vm(2, *per_step),
            vm(STEPS, *plane),
            pltpu.VMEM((2,) + plane, jnp.int32),
            vm(6, 2, *plane),
            vm(2, *plane),
            vm(*field),
            vm(*per_step),
            vm(*per_step),
            pltpu.SemaphoreType.DMA,
            dma(TICKS),
            dma(STEPS),
            dma(STEPS),
            pltpu.SemaphoreType.DMA,
            pltpu.SemaphoreType.DMA,
            dma(TICKS, 2, STEPS),
            dma(TICKS, 2, STEPS),
            dma(STEPS + 1),
            dma(6),
            dma(8 + TICKS + 2),
            dma(TICKS, 2, STEPS),
            dma(TICKS, 2, STEPS),
            dma(STEPS),
            dma(STEPS),
            pltpu.SemaphoreType.DMA,
            dma(TICKS, STEPS),
            dma(TICKS, STEPS),
        ],
        compiler_params=pltpu.CompilerParams(collective_id=0, has_side_effects=True),
    )(cond_table, cap_table, fields, labels, traces, new_guess)
    return pl.pallas_call(
        deliver,
        out_shape=(
            jax.ShapeDtypeStruct((1, 2) + plane, F32),
            jax.ShapeDtypeStruct((1, 1, STEPS) + plane, F32),
        ),
        in_specs=[any_spec] * 2,
        out_specs=(any_spec, any_spec),
        scratch_shapes=[vm(2 + STEPS, *plane), dma(2 + STEPS), dma(2 + STEPS)],
    )(*results)


def solution(mesh):
    return jax.shard_map(
        local,
        mesh=mesh,
        in_specs=(
            P("iter", "sub", None, None),
            P("sub", None, None),
            P("iter", "sub", None, None, None),
            P(None, "sub", None, None, None),
            P(),
            P(),
        ),
        out_specs=(P("iter", "sub", None, None), P("iter", "sub", None, None, None)),
        check_vma=False,
    )
```

```python
import functools

import jax
import jax.numpy as jnp
from jax import lax
from jax.experimental import pallas as pl
from jax.experimental.pallas import tpu as pltpu
from jax.sharding import PartitionSpec as P

MESH = pl.DeviceIdType.MESH
TICKS = 3
STEPS = 4
NY = 128
NZ = 128
PAD = 8
ROWS = NY + 2 * PAD
CHUNK = 32
SPAN = 8
F32 = jnp.float32


def harmonic(first, second):
    return 2.0 * first * second / (first + second)


def sweep(source, target, rhs, coeff, extra=None):
    for plane in range(2):
        for row in range(0, NY, CHUNK):
            here = slice(row, row + CHUNK)
            base = PAD + row
            v = source[plane, base : base + CHUNK, :]
            out = rhs[plane, here, :]
            out = out + coeff[0, plane, here, :] * source[1 - plane, base : base + CHUNK, :]
            out = out + coeff[1, plane, here, :] * source[plane, base - 1 : base - 1 + CHUNK, :]
            out = out + coeff[2, plane, here, :] * source[plane, base + 1 : base + 1 + CHUNK, :]
            out = out + coeff[3, plane, here, :] * pltpu.roll(v, 1, 1)
            out = out + coeff[4, plane, here, :] * pltpu.roll(v, NZ - 1, 1)
            target[plane, base : base + CHUNK, :] = out
            if extra is not None:
                extra(plane, here, out)


def kernel(
    cond_hbm, cap_hbm, fields, labels, traces, guess,
    out_u, out_h,
    cond_ref, cap_ref,
    stage_lab, stage_u, stage_h, lab, u, h_right, h_left, guess_right, guess_left,
    psi, buf_a, buf_b, rhs, co_d, co_n, end, inv_n,
    qs, qr, ps, pr, back,
    lab_o, co_o, inv_o, psi_o, jump_in, jump_far,
    lab_sem, u_sem, h_sem, hl_sem, gr_sem, gl_sem,
    q_sem, p_sem, out_sem, load_sem, send_sem, qs_sem, ps_sem, hs_sem, bs_sem,
    lab_o_sem, far_sem, in_sem,
):
    sub = lax.axis_index("sub")
    it = lax.axis_index("iter")
    pair = sub // 2
    xl = sub % 2
    xh = it // 2
    core = it % 2
    ring = 2 * xh + xl
    slab = 2 * pair + core
    pairs = lax.axis_size("sub") // 2
    has_left = slab > 0
    has_right = slab < 2 * pairs - 1
    swapped = xl != core
    stays = xl == core
    takes_guess = xh == 1

    outer_right = jnp.logical_and(jnp.logical_and(core == 1, has_right), pair % SPAN == SPAN - 1)
    outer_left = jnp.logical_and(jnp.logical_and(core == 0, has_left), pair % SPAN == 0)
    long = jnp.logical_or(outer_right, outer_left)
    short = jnp.logical_not(long)
    exists = (has_left, has_right)
    restart = [None] + [ring == 4 - tick for tick in range(1, TICKS)]
    useful = [ring != 3 - tick for tick in range(TICKS - 1)] + [ring >= 0]
    q_wait = (
        jnp.logical_and(has_left, jnp.logical_not(outer_right)),
        jnp.logical_and(has_right, jnp.logical_not(outer_left)),
    )
    p_uses = (
        jnp.logical_and(has_left, jnp.logical_not(outer_left)),
        jnp.logical_and(has_right, jnp.logical_not(outer_right)),
    )
    outer_id = {"sub": sub + 4 * core - 2, "iter": it + 1 - 2 * core}

    right_id = {"sub": sub + 2 * core, "iter": it + 1 - 2 * core}
    left_id = {"sub": sub - 2 * (1 - core), "iter": it + 1 - 2 * core}
    partner_id = {"sub": sub + 1 - 2 * xl, "iter": it + 1 - 2 * core}
    down = (ring + 3) % 4
    up = (ring + 1) % 4
    down_id = {"sub": 2 * pair + down % 2, "iter": 2 * (down // 2) + core}
    up_id = {"sub": 2 * pair + up % 2, "iter": 2 * (up // 2) + core}
    other = (ring + 1 + 2 * core) % 4
    other_id = {"sub": 2 * pair + other % 2, "iter": 2 * (other // 2) + 1 - core}
    home_id = {"sub": 2 * pair + core, "iter": (ring + 2) % 4}
    source_ring = (it + 2) % 4
    source_id = {"sub": 2 * pair + source_ring % 2, "iter": 2 * (source_ring // 2) + xl}

    def remote(src, dst, send, recv, device):
        return pltpu.make_async_remote_copy(
            src_ref=src, dst_ref=dst, send_sem=send, recv_sem=recv, device_id=device, device_id_type=MESH
        )

    inner = pl.ds(PAD, NY)

    zero_pad = jnp.zeros((2, PAD, NZ), F32)
    for ref in (buf_a, buf_b, psi, psi_o):
        ref[:, 0:PAD, :] = zero_pad
        ref[:, PAD + NY : ROWS, :] = zero_pad
    for tick in range(TICKS):
        u[tick, :, 0:PAD, :] = zero_pad
        u[tick, :, PAD + NY : ROWS, :] = zero_pad

    barrier = pltpu.get_barrier_semaphore()

    def greet(device):
        pl.semaphore_signal(barrier, inc=1, device_id=device, device_id_type=MESH)

    pl.when(has_left)(lambda: greet(left_id))
    pl.when(has_right)(lambda: greet(right_id))
    pl.when(swapped)(lambda: greet(partner_id))
    pl.when(swapped)(lambda: greet(other_id))
    greet(up_id)
    greet(source_id)

    def loads(d_h, d_lab, d_u):
        return [
            pltpu.make_async_copy(traces.at[0, 0, 0:1], d_h.at[0:1], load_sem.at[0]),
            pltpu.make_async_copy(labels, d_lab, load_sem.at[1]),
            pltpu.make_async_copy(fields.at[0], d_u, load_sem.at[2]),
            pltpu.make_async_copy(traces.at[0, 0, 1:STEPS], d_h.at[1:STEPS], load_sem.at[3]),
        ]

    keep = loads(h_right, lab, u.at[0, :, inner, :])
    pass_on = loads(stage_h, stage_lab, stage_u)
    keep_guess = pltpu.make_async_copy(guess.at[1 - xl, 0], guess_right, gr_sem)

    tables = [
        pltpu.make_async_copy(cond_hbm, cond_ref, load_sem.at[4]),
        pltpu.make_async_copy(cap_hbm, cap_ref, load_sem.at[5]),
    ]
    for copy in tables:
        copy.start()

    @pl.when(stays)
    def _():
        for copy in keep:
            copy.start()

    @pl.when(swapped)
    def _():
        for copy in pass_on:
            copy.start()

    @pl.when(jnp.logical_and(stays, takes_guess))
    def _():
        keep_guess.start()

    peers = 2 + 2 * ((xl + core) % 2) + jnp.where(has_left, 1, 0) + jnp.where(has_right, 1, 0)
    pl.semaphore_wait(barrier, peers)

    swap_h = [
        remote(stage_h.at[n], h_right.at[n], send_sem.at[n], h_sem.at[n], partner_id) for n in range(STEPS)
    ]
    swap_lab = remote(stage_lab, lab, send_sem.at[4], lab_sem, other_id)
    swap_u = remote(stage_u, u.at[0, :, inner, :], send_sem.at[5], u_sem.at[0], partner_id)
    swap_guess = remote(guess.at[xl, 0], guess_right, send_sem.at[6], gr_sem, partner_id)
    pass_guess = remote(guess_right, guess_left, send_sem.at[7], gl_sem, right_id)
    move_u = [
        remote(u.at[t, :, inner, :], u.at[t + 1, :, inner, :], send_sem.at[8 + t], u_sem.at[t + 1], down_id)
        for t in range(TICKS - 1)
    ]
    home_u = remote(u.at[TICKS - 1, :, inner, :], out_u.at[0], send_sem.at[8 + TICKS], out_sem.at[STEPS], home_id)

    def pass_h(n):
        return remote(h_right.at[n], h_left.at[n], hs_sem.at[n], hl_sem.at[n], right_id)

    sides = (left_id, right_id)

    def send_q(side, t, n):
        return remote(qs.at[side, t, n], qr.at[1 - side, t, n], qs_sem.at[t, side, n], q_sem.at[t, 1 - side, n], sides[side])

    def send_p(side, t, n):
        return remote(ps.at[side, t, n], pr.at[1 - side, t, n], ps_sem.at[t, side, n], p_sem.at[t, 1 - side, n], sides[side])

    def got_q(side, t, n):
        return remote(qs.at[side, t, n], qr.at[side, t, n], qs_sem.at[t, side, n], q_sem.at[t, side, n], left_id)

    def got_p(side, t, n):
        return remote(ps.at[side, t, n], pr.at[side, t, n], ps_sem.at[t, side, n], p_sem.at[t, side, n], left_id)

    def send_jump(t, n):
        return remote(jump_in.at[t, n], jump_far.at[t, n], in_sem.at[t, n], far_sem.at[t, n], outer_id)

    send_lab = remote(lab, lab_o, send_sem.at[8 + TICKS + 1], lab_o_sem, outer_id)

    def send_home(n):
        return remote(back.at[n], out_h.at[0, 0, n], bs_sem.at[n], out_sem.at[n], home_id)

    @pl.when(swapped)
    def _():
        pass_on[0].wait()
        swap_h[0].start()
        pass_on[1].wait()
        swap_lab.start()
        pass_on[3].wait()
        for copy in swap_h[1:]:
            copy.start()
        pass_on[2].wait()
        swap_u.start()

    @pl.when(jnp.logical_and(swapped, takes_guess))
    def _():
        swap_guess.start()

    @pl.when(stays)
    def _():
        keep[0].wait()
        keep[3].wait()

    for n in range(STEPS):
        pl.when(swapped)(swap_h[n].wait_recv)
        pl.when(has_right)(pass_h(n).start)

    @pl.when(jnp.logical_and(stays, takes_guess))
    def _():
        keep_guess.wait()
        pl.when(has_right)(pass_guess.start)

    @pl.when(jnp.logical_not(has_right))
    def _():
        h_right[...] = jnp.zeros((STEPS, NY, NZ), F32)

    @pl.when(jnp.logical_not(has_left))
    def _():
        h_left[...] = jnp.zeros((STEPS, NY, NZ), F32)

    pl.when(stays)(keep[1].wait)
    pl.when(swapped)(swap_lab.wait_recv)

    for copy in tables:
        copy.wait()

    def pick(table, value):
        result = jnp.full(value.shape, table[0], F32)
        for cls in range(1, 4):
            result = jnp.where(value == cls, table[cls], result)
        return result

    pl.when(long)(send_lab.start)
    lane = lax.broadcasted_iota(jnp.int32, (CHUNK, NZ), 1)
    line = lax.broadcasted_iota(jnp.int32, (CHUNK, NZ), 0)

    def coefficients(label, scratch, edges, own):
        for plane in range(2):
            for row in range(0, NY, CHUNK):
                scratch[plane, PAD + row : PAD + row + CHUNK, :] = pick(cond_ref, label[plane, row : row + CHUNK, :])
        for plane in range(2):
            for row in range(0, NY, CHUNK):
                here = slice(row, row + CHUNK)
                base = PAD + row
                k = scratch[plane, base : base + CHUNK, :]
                twice = 2.0 * k
                face_x = harmonic(k, scratch[1 - plane, base : base + CHUNK, :])
                face_u = harmonic(k, scratch[plane, base - 1 : base - 1 + CHUNK, :])
                face_d = harmonic(k, scratch[plane, base + 1 : base + 1 + CHUNK, :])
                face_l = jnp.where(lane == 0, 0.0, harmonic(k, pltpu.roll(k, 1, 1)))
                face_r = jnp.where(lane == NZ - 1, 0.0, harmonic(k, pltpu.roll(k, NZ - 1, 1)))
                side_u = jnp.where(line + row == 0, twice, face_u) if row == 0 else face_u
                side_d = jnp.where(line + row == NY - 1, twice, face_d) if row + CHUNK == NY else face_d
                side_l = jnp.where(lane == 0, twice, face_l)
                side_r = jnp.where(lane == NZ - 1, twice, face_r)
                capacity = pick(cap_ref, label[plane, here, :])
                common = capacity + face_x + side_u + side_d + side_l + side_r
                faces = (face_x, face_u, face_d, face_l, face_r, capacity)
                if own:
                    inv_neu = 1.0 / jnp.where(edges[plane], common, common + twice)
                    inv_dir = 1.0 / (common + twice)
                    for j, face in enumerate(faces):
                        co_d[j, plane, here, :] = face * inv_dir
                    co_d[6, plane, here, :] = twice * inv_dir
                    end[plane, here, :] = twice
                else:
                    inv_neu = 1.0 / common
                for j, face in enumerate(faces):
                    (co_n if own else co_o)[j, plane, here, :] = face * inv_neu
                (inv_n if own else inv_o)[plane, here, :] = inv_neu

    coefficients(lab, buf_a, exists, True)

    pl.when(stays)(keep[2].wait)
    pl.when(swapped)(swap_u.wait_recv)

    last = TICKS - 1

    def inner_jump(t, n, carry):
        got_q(1 - core, t, n).wait_recv()
        for row in range(0, NY, CHUNK):
            here = slice(row, row + CHUNK)
            jump_in[t, n, here, :] = qs[1 - core, t, n, here, :] + qr[1 - core, t, n, here, :]
        if t < last:
            send_jump(t, n).start()
        else:
            pl.when(outer_left)(send_jump(t, n).start)
        return carry

    def outer(t, n):
        send_jump(t, n).wait_recv()
        near, far = 1 - core, core
        for row in range(0, NY, CHUNK):
            here = slice(row, row + CHUNK)
            rows = slice(PAD + row, PAD + row + CHUNK)
            jump = qs[core, t, n, here, :] + qr[core, t, n, here, :]
            rhs[near, here, :] = inv_o[near, here, :] * jump + co_o[5, near, here, :] * psi_o[near, rows, :]
            rhs[far, here, :] = (
                inv_o[far, here, :] * jump_far[t, n, here, :] + co_o[5, far, here, :] * psi_o[far, rows, :]
            )
        sweep(psi_o, buf_a, rhs, co_o)
        sweep(buf_a, buf_b, rhs, co_o)
        sweep(buf_b, psi_o, rhs, co_o)
        for row in range(0, NY, CHUNK):
            pr[core, t, n, row : row + CHUNK, :] = psi_o[near, PAD + row : PAD + row + CHUNK, :]

    def finish(n, carry, solve=True):
        if solve:
            pl.when(outer_right)(lambda: outer(last, n))
        pl.when(p_uses[1])(got_p(1, last, n).wait_recv)
        for row in range(0, NY, CHUNK):
            here = slice(row, row + CHUNK)
            new = h_right[n, here, :] + 0.25 * (ps[1, last, n, here, :] + pr[1, last, n, here, :])
            back[n, here, :] = jnp.where(has_right, new, 0.0)
        send_home(n).start()
        return carry

    for tick in range(TICKS):
        state = u.at[tick]
        if tick > 0:
            pl.when(jnp.logical_and(restart[tick], has_left))(pass_guess.wait_recv)

        def dirichlet(n, carry, tick=tick, state=state):
            if tick == 0:
                pl.when(has_left)(pass_h(n).wait_recv)
            else:
                if tick == 1:
                    pl.when(has_right)(pass_h(n).wait_send)

                @pl.when(useful[tick - 1])
                def _():
                    pl.when(long)(lambda: outer(tick - 1, n))
                    for side, trace in enumerate((h_left, h_right)):
                        pl.when(p_uses[side])(got_p(side, tick - 1, n).wait_recv)
                        for row in range(0, NY, CHUNK):
                            here = slice(row, row + CHUNK)
                            both = ps[side, tick - 1, n, here, :] + pr[side, tick - 1, n, here, :]
                            new = trace[n, here, :] + 0.25 * both
                            trace[n, here, :] = jnp.where(exists[side], new, 0.0)

                @pl.when(restart[tick])
                def _():
                    for side, (trace, taken) in enumerate(((h_left, guess_left), (h_right, guess_right))):
                        for row in range(0, NY, CHUNK):
                            here = slice(row, row + CHUNK)
                            trace[n, here, :] = jnp.where(exists[side], taken[n, here, :], 0.0)

                pl.when(n == 0)(move_u[tick - 1].wait_recv)

            for plane, trace in enumerate((h_left, h_right)):
                for row in range(0, NY, CHUNK):
                    here = slice(row, row + CHUNK)
                    rhs[plane, here, :] = (
                        co_d[5, plane, here, :] * state[plane, PAD + row : PAD + row + CHUNK, :]
                        + co_d[6, plane, here, :] * trace[n, here, :]
                    )

            def flux(plane, here, value):
                trace = (h_left, h_right)[plane]
                qs[plane, tick, n, here, :] = end[plane, here, :] * (value - trace[n, here, :])

            sweep(state, buf_a, rhs, co_d)
            sweep(buf_a, buf_b, rhs, co_d)
            sweep(buf_b, state, rhs, co_d, flux)
            pl.when(jnp.logical_and(has_right, useful[tick]))(send_q(1, tick, n).start)
            pl.when(jnp.logical_and(has_left, useful[tick]))(send_q(0, tick, n).start)
            return carry

        lax.fori_loop(0, STEPS, dirichlet, 0)
        if tick + 1 < TICKS:
            move_u[tick].start()
        else:
            home_u.start()
        if tick + 1 < TICKS:

            @pl.when(jnp.logical_and(swapped, restart[tick + 1]))
            def _():
                swap_guess.wait_recv()
                pl.when(has_right)(pass_guess.start)

        @pl.when(jnp.logical_and(long, useful[tick]))
        def _():
            lax.fori_loop(0, STEPS, functools.partial(inner_jump, tick), 0)

        def neumann(n, carry, tick=tick, first=False):
            for side in range(2):
                pl.when(q_wait[side])(got_q(side, tick, n).wait_recv)
            for plane in range(2):
                for row in range(0, NY, CHUNK):
                    here = slice(row, row + CHUNK)
                    jump = qs[plane, tick, n, here, :] + qr[plane, tick, n, here, :]
                    value = inv_n[plane, here, :] * jnp.where(exists[plane], jump, 0.0)
                    if not first:
                        value = value + co_n[5, plane, here, :] * psi[plane, PAD + row : PAD + row + CHUNK, :]
                    rhs[plane, here, :] = value
                    if first:
                        buf_a[plane, PAD + row : PAD + row + CHUNK, :] = value

            def ends(plane, here, value):
                ps[plane, tick, n, here, :] = value

            if not first:
                sweep(psi, buf_a, rhs, co_n)
            sweep(buf_a, buf_b, rhs, co_n)
            sweep(buf_b, psi, rhs, co_n, ends)
            pl.when(p_uses[0])(send_p(0, tick, n).start)
            if tick + 1 < TICKS:
                pl.when(p_uses[1])(send_p(1, tick, n).start)
            elif not first:
                @pl.when(core == 0)
                def _():
                    finish(n - 1, 0, False)

            return carry

        @pl.when(useful[tick])
        def _():
            neumann(0, 0, first=True)

        @pl.when(long)
        def _():
            if tick == 0:
                send_lab.wait_recv()
                coefficients(lab_o, psi_o, None, False)
            psi_o[:, PAD : PAD + NY, :] = jnp.zeros((2, NY, NZ), F32)

        @pl.when(useful[tick])
        def _():
            lax.fori_loop(1, STEPS, neumann, 0)


    @pl.when(core == 1)
    def _():
        lax.fori_loop(0, STEPS, finish, 0)

    @pl.when(core == 0)
    def _():
        finish(STEPS - 1, 0, False)


    @pl.when(swapped)
    def _():
        for copy in swap_h:
            copy.wait_send()
        swap_lab.wait_send()
        swap_u.wait_send()

    pl.when(jnp.logical_and(swapped, takes_guess))(swap_guess.wait_send)
    pl.when(jnp.logical_and(takes_guess, has_right))(pass_guess.wait_send)
    for copy in move_u:
        copy.wait_send()
    home_u.wait_send()

    for side in range(2):

        @pl.when(exists[side])
        def _():
            for n in range(STEPS):
                for t in range(TICKS):
                    pl.when(useful[t])(send_q(side, t, n).wait_send)

        @pl.when(p_uses[side])
        def _():
            for n in range(STEPS):
                for t in range(TICKS if side == 0 else last):
                    pl.when(useful[t])(send_p(side, t, n).wait_send)

    @pl.when(long)
    def _():
        send_lab.wait_send()
        for n in range(STEPS):
            for t in range(last):
                pl.when(useful[t])(send_jump(t, n).wait_send)

    @pl.when(outer_left)
    def _():
        for n in range(STEPS):
            send_jump(last, n).wait_send()

    for n in range(STEPS):
        send_home(n).wait_send()
    home_u.wait_recv()
    for n in range(STEPS):
        send_home(n).wait_recv()


def deliver(field, trace, out_field, out_trace, block, in_sem, out_sem):
    pieces = [(field.at[0, i], out_field.at[0, i]) for i in range(2)]
    pieces += [(trace.at[0, 0, n], out_trace.at[0, 0, n]) for n in range(STEPS)]
    loads = [pltpu.make_async_copy(src, block.at[i], in_sem.at[i]) for i, (src, _) in enumerate(pieces)]
    stores = [pltpu.make_async_copy(block.at[i], dst, out_sem.at[i]) for i, (_, dst) in enumerate(pieces)]
    for copy in loads:
        copy.start()
    for load, store in zip(loads, stores):
        load.wait()
        store.start()
    for store in stores:
        store.wait()


def local(fields, labels, traces, new_guess, cond_table, cap_table):
    plane = (NY, NZ)
    field = (2, ROWS, NZ)
    vm = lambda *shape: pltpu.VMEM(shape, F32)
    dma = lambda *shape: pltpu.SemaphoreType.DMA(shape)
    any_spec = pl.BlockSpec(memory_space=pl.ANY)
    hbm = pl.BlockSpec(memory_space=pltpu.HBM)
    per_step = (TICKS, STEPS) + plane
    results = pl.pallas_call(
        kernel,
        out_shape=(
            jax.ShapeDtypeStruct((1, 2) + plane, F32),
            jax.ShapeDtypeStruct((1, 1, STEPS) + plane, F32),
        ),
        in_specs=[hbm] * 6,
        out_specs=(any_spec, any_spec),
        scratch_shapes=[
            pltpu.SMEM((4,), F32),
            pltpu.SMEM((4,), F32),
            pltpu.VMEM((2,) + plane, jnp.int32),
            vm(2, *plane),
            vm(STEPS, *plane),
            pltpu.VMEM((2,) + plane, jnp.int32),
            vm(TICKS, *field),
            vm(STEPS, *plane),
            vm(STEPS, *plane),
            vm(STEPS, *plane),
            vm(STEPS, *plane),
            vm(*field),
            vm(*field),
            vm(*field),
            vm(2, *plane),
            vm(7, 2, *plane),
            vm(6, 2, *plane),
            vm(2, *plane),
            vm(2, *plane),
            vm(2, *per_step),
            vm(2, *per_step),
            vm(2, *per_step),
            vm(2, *per_step),
            vm(STEPS, *plane),
            pltpu.VMEM((2,) + plane, jnp.int32),
            vm(6, 2, *plane),
            vm(2, *plane),
            vm(*field),
            vm(*per_step),
            vm(*per_step),
            pltpu.SemaphoreType.DMA,
            dma(TICKS),
            dma(STEPS),
            dma(STEPS),
            pltpu.SemaphoreType.DMA,
            pltpu.SemaphoreType.DMA,
            dma(TICKS, 2, STEPS),
            dma(TICKS, 2, STEPS),
            dma(STEPS + 1),
            dma(6),
            dma(8 + TICKS + 2),
            dma(TICKS, 2, STEPS),
            dma(TICKS, 2, STEPS),
            dma(STEPS),
            dma(STEPS),
            pltpu.SemaphoreType.DMA,
            dma(TICKS, STEPS),
            dma(TICKS, STEPS),
        ],
        compiler_params=pltpu.CompilerParams(collective_id=0, has_side_effects=True),
    )(cond_table, cap_table, fields, labels, traces, new_guess)
    return pl.pallas_call(
        deliver,
        out_shape=(
            jax.ShapeDtypeStruct((1, 2) + plane, F32),
            jax.ShapeDtypeStruct((1, 1, STEPS) + plane, F32),
        ),
        in_specs=[any_spec] * 2,
        out_specs=(any_spec, any_spec),
        scratch_shapes=[vm(2 + STEPS, *plane), dma(2 + STEPS), dma(2 + STEPS)],
    )(*results)


def solution(mesh):
    return jax.shard_map(
        local,
        mesh=mesh,
        in_specs=(
            P("iter", "sub", None, None),
            P("sub", None, None),
            P("iter", "sub", None, None, None),
            P(None, "sub", None, None, None),
            P(),
            P(),
        ),
        out_specs=(P("iter", "sub", None, None), P("iter", "sub", None, None, None)),
        check_vma=False,
    )
```

```python
import functools

import jax
import jax.numpy as jnp
from jax import lax
from jax.experimental import pallas as pl
from jax.experimental.pallas import tpu as pltpu
from jax.sharding import PartitionSpec as P

MESH = pl.DeviceIdType.MESH
TICKS = 3
STEPS = 4
NY = 128
NZ = 128
PAD = 8
ROWS = NY + 2 * PAD
CHUNK = 32
SPAN = 8
F32 = jnp.float32


def harmonic(first, second):
    return 2.0 * first * second / (first + second)


def sweep(source, target, rhs, coeff, extra=None):
    for plane in range(2):
        for row in range(0, NY, CHUNK):
            here = slice(row, row + CHUNK)
            base = PAD + row
            v = source[plane, base : base + CHUNK, :]
            out = rhs[plane, here, :]
            out = out + coeff[0, plane, here, :] * source[1 - plane, base : base + CHUNK, :]
            out = out + coeff[1, plane, here, :] * source[plane, base - 1 : base - 1 + CHUNK, :]
            out = out + coeff[2, plane, here, :] * source[plane, base + 1 : base + 1 + CHUNK, :]
            out = out + coeff[3, plane, here, :] * pltpu.roll(v, 1, 1)
            out = out + coeff[4, plane, here, :] * pltpu.roll(v, NZ - 1, 1)
            target[plane, base : base + CHUNK, :] = out
            if extra is not None:
                extra(plane, here, out)


def kernel(
    cond_hbm, cap_hbm, fields, labels, traces, guess,
    out_u, out_h,
    cond_ref, cap_ref,
    stage_lab, stage_u, stage_h, lab, u, h_right, h_left, guess_right, guess_left,
    psi, buf_a, buf_b, rhs, co_d, co_n, end, inv_n,
    qs, qr, ps, pr, back,
    lab_o, co_o, inv_o, psi_o, jump_in, jump_far,
    lab_sem, u_sem, h_sem, hl_sem, gr_sem, gl_sem,
    q_sem, p_sem, out_sem, load_sem, send_sem, qs_sem, ps_sem, hs_sem, bs_sem,
    lab_o_sem, far_sem, in_sem,
):
    sub = lax.axis_index("sub")
    it = lax.axis_index("iter")
    pair = sub // 2
    xl = sub % 2
    xh = it // 2
    core = it % 2
    ring = 2 * xh + xl
    slab = 2 * pair + core
    pairs = lax.axis_size("sub") // 2
    has_left = slab > 0
    has_right = slab < 2 * pairs - 1
    swapped = xl != core
    stays = xl == core
    takes_guess = xh == 1

    outer_right = jnp.logical_and(jnp.logical_and(core == 1, has_right), pair % SPAN == SPAN - 1)
    outer_left = jnp.logical_and(jnp.logical_and(core == 0, has_left), pair % SPAN == 0)
    long = jnp.logical_or(outer_right, outer_left)
    lagging = jnp.logical_and(core == 0, jnp.logical_not(outer_left))
    short = jnp.logical_not(long)
    exists = (has_left, has_right)
    restart = [None] + [ring == 4 - tick for tick in range(1, TICKS)]
    useful = [ring != 3 - tick for tick in range(TICKS - 1)] + [ring >= 0]
    q_wait = (
        jnp.logical_and(has_left, jnp.logical_not(outer_right)),
        jnp.logical_and(has_right, jnp.logical_not(outer_left)),
    )
    p_uses = (
        jnp.logical_and(has_left, jnp.logical_not(outer_left)),
        jnp.logical_and(has_right, jnp.logical_not(outer_right)),
    )
    outer_id = {"sub": sub + 4 * core - 2, "iter": it + 1 - 2 * core}

    right_id = {"sub": sub + 2 * core, "iter": it + 1 - 2 * core}
    left_id = {"sub": sub - 2 * (1 - core), "iter": it + 1 - 2 * core}
    partner_id = {"sub": sub + 1 - 2 * xl, "iter": it + 1 - 2 * core}
    down = (ring + 3) % 4
    up = (ring + 1) % 4
    down_id = {"sub": 2 * pair + down % 2, "iter": 2 * (down // 2) + core}
    up_id = {"sub": 2 * pair + up % 2, "iter": 2 * (up // 2) + core}
    other = (ring + 1 + 2 * core) % 4
    other_id = {"sub": 2 * pair + other % 2, "iter": 2 * (other // 2) + 1 - core}
    home_id = {"sub": 2 * pair + core, "iter": (ring + 2) % 4}
    source_ring = (it + 2) % 4
    source_id = {"sub": 2 * pair + source_ring % 2, "iter": 2 * (source_ring // 2) + xl}

    def remote(src, dst, send, recv, device):
        return pltpu.make_async_remote_copy(
            src_ref=src, dst_ref=dst, send_sem=send, recv_sem=recv, device_id=device, device_id_type=MESH
        )

    inner = pl.ds(PAD, NY)

    zero_pad = jnp.zeros((2, PAD, NZ), F32)
    for ref in (buf_a, buf_b, psi, psi_o):
        ref[:, 0:PAD, :] = zero_pad
        ref[:, PAD + NY : ROWS, :] = zero_pad
    for tick in range(TICKS):
        u[tick, :, 0:PAD, :] = zero_pad
        u[tick, :, PAD + NY : ROWS, :] = zero_pad

    barrier = pltpu.get_barrier_semaphore()

    def greet(device):
        pl.semaphore_signal(barrier, inc=1, device_id=device, device_id_type=MESH)

    pl.when(has_left)(lambda: greet(left_id))
    pl.when(has_right)(lambda: greet(right_id))
    pl.when(swapped)(lambda: greet(partner_id))
    pl.when(swapped)(lambda: greet(other_id))
    greet(up_id)
    greet(source_id)

    def loads(d_h, d_lab, d_u):
        return [
            pltpu.make_async_copy(traces.at[0, 0, 0:1], d_h.at[0:1], load_sem.at[0]),
            pltpu.make_async_copy(labels, d_lab, load_sem.at[1]),
            pltpu.make_async_copy(fields.at[0], d_u, load_sem.at[2]),
            pltpu.make_async_copy(traces.at[0, 0, 1:STEPS], d_h.at[1:STEPS], load_sem.at[3]),
        ]

    keep = loads(h_right, lab, u.at[0, :, inner, :])
    pass_on = loads(stage_h, stage_lab, stage_u)
    keep_guess = pltpu.make_async_copy(guess.at[1 - xl, 0], guess_right, gr_sem)

    tables = [
        pltpu.make_async_copy(cond_hbm, cond_ref, load_sem.at[4]),
        pltpu.make_async_copy(cap_hbm, cap_ref, load_sem.at[5]),
    ]
    for copy in tables:
        copy.start()

    @pl.when(stays)
    def _():
        for copy in keep:
            copy.start()

    @pl.when(swapped)
    def _():
        for copy in pass_on:
            copy.start()

    @pl.when(jnp.logical_and(stays, takes_guess))
    def _():
        keep_guess.start()

    peers = 2 + 2 * ((xl + core) % 2) + jnp.where(has_left, 1, 0) + jnp.where(has_right, 1, 0)
    pl.semaphore_wait(barrier, peers)

    swap_h = [
        remote(stage_h.at[n], h_right.at[n], send_sem.at[n], h_sem.at[n], partner_id) for n in range(STEPS)
    ]
    swap_lab = remote(stage_lab, lab, send_sem.at[4], lab_sem, other_id)
    swap_u = remote(stage_u, u.at[0, :, inner, :], send_sem.at[5], u_sem.at[0], partner_id)
    swap_guess = remote(guess.at[xl, 0], guess_right, send_sem.at[6], gr_sem, partner_id)
    pass_guess = remote(guess_right, guess_left, send_sem.at[7], gl_sem, right_id)
    move_u = [
        remote(u.at[t, :, inner, :], u.at[t + 1, :, inner, :], send_sem.at[8 + t], u_sem.at[t + 1], down_id)
        for t in range(TICKS - 1)
    ]
    home_u = remote(u.at[TICKS - 1, :, inner, :], out_u.at[0], send_sem.at[8 + TICKS], out_sem.at[STEPS], home_id)

    def pass_h(n):
        return remote(h_right.at[n], h_left.at[n], hs_sem.at[n], hl_sem.at[n], right_id)

    sides = (left_id, right_id)

    def send_q(side, t, n):
        return remote(qs.at[side, t, n], qr.at[1 - side, t, n], qs_sem.at[t, side, n], q_sem.at[t, 1 - side, n], sides[side])

    def send_p(side, t, n):
        return remote(ps.at[side, t, n], pr.at[1 - side, t, n], ps_sem.at[t, side, n], p_sem.at[t, 1 - side, n], sides[side])

    def got_q(side, t, n):
        return remote(qs.at[side, t, n], qr.at[side, t, n], qs_sem.at[t, side, n], q_sem.at[t, side, n], left_id)

    def got_p(side, t, n):
        return remote(ps.at[side, t, n], pr.at[side, t, n], ps_sem.at[t, side, n], p_sem.at[t, side, n], left_id)

    def send_jump(t, n):
        return remote(jump_in.at[t, n], jump_far.at[t, n], in_sem.at[t, n], far_sem.at[t, n], outer_id)

    send_lab = remote(lab, lab_o, send_sem.at[8 + TICKS + 1], lab_o_sem, outer_id)

    def send_home(n):
        return remote(back.at[n], out_h.at[0, 0, n], bs_sem.at[n], out_sem.at[n], home_id)

    @pl.when(swapped)
    def _():
        pass_on[0].wait()
        swap_h[0].start()
        pass_on[1].wait()
        swap_lab.start()
        pass_on[3].wait()
        for copy in swap_h[1:]:
            copy.start()
        pass_on[2].wait()
        swap_u.start()

    @pl.when(jnp.logical_and(swapped, takes_guess))
    def _():
        swap_guess.start()

    @pl.when(stays)
    def _():
        keep[0].wait()
        keep[3].wait()

    for n in range(STEPS):
        pl.when(swapped)(swap_h[n].wait_recv)
        pl.when(has_right)(pass_h(n).start)

    @pl.when(jnp.logical_and(stays, takes_guess))
    def _():
        keep_guess.wait()
        pl.when(has_right)(pass_guess.start)

    @pl.when(jnp.logical_not(has_right))
    def _():
        h_right[...] = jnp.zeros((STEPS, NY, NZ), F32)

    @pl.when(jnp.logical_not(has_left))
    def _():
        h_left[...] = jnp.zeros((STEPS, NY, NZ), F32)

    pl.when(stays)(keep[1].wait)
    pl.when(swapped)(swap_lab.wait_recv)

    for copy in tables:
        copy.wait()

    def pick(table, value):
        result = jnp.full(value.shape, table[0], F32)
        for cls in range(1, 4):
            result = jnp.where(value == cls, table[cls], result)
        return result

    pl.when(long)(send_lab.start)
    lane = lax.broadcasted_iota(jnp.int32, (CHUNK, NZ), 1)
    line = lax.broadcasted_iota(jnp.int32, (CHUNK, NZ), 0)

    def coefficients(label, scratch, edges, own):
        for plane in range(2):
            for row in range(0, NY, CHUNK):
                scratch[plane, PAD + row : PAD + row + CHUNK, :] = pick(cond_ref, label[plane, row : row + CHUNK, :])
        for plane in range(2):
            for row in range(0, NY, CHUNK):
                here = slice(row, row + CHUNK)
                base = PAD + row
                k = scratch[plane, base : base + CHUNK, :]
                twice = 2.0 * k
                face_x = harmonic(k, scratch[1 - plane, base : base + CHUNK, :])
                face_u = harmonic(k, scratch[plane, base - 1 : base - 1 + CHUNK, :])
                face_d = harmonic(k, scratch[plane, base + 1 : base + 1 + CHUNK, :])
                face_l = jnp.where(lane == 0, 0.0, harmonic(k, pltpu.roll(k, 1, 1)))
                face_r = jnp.where(lane == NZ - 1, 0.0, harmonic(k, pltpu.roll(k, NZ - 1, 1)))
                side_u = jnp.where(line + row == 0, twice, face_u) if row == 0 else face_u
                side_d = jnp.where(line + row == NY - 1, twice, face_d) if row + CHUNK == NY else face_d
                side_l = jnp.where(lane == 0, twice, face_l)
                side_r = jnp.where(lane == NZ - 1, twice, face_r)
                capacity = pick(cap_ref, label[plane, here, :])
                common = capacity + face_x + side_u + side_d + side_l + side_r
                faces = (face_x, face_u, face_d, face_l, face_r, capacity)
                if own:
                    inv_neu = 1.0 / jnp.where(edges[plane], common, common + twice)
                    inv_dir = 1.0 / (common + twice)
                    for j, face in enumerate(faces):
                        co_d[j, plane, here, :] = face * inv_dir
                    co_d[6, plane, here, :] = twice * inv_dir
                    end[plane, here, :] = twice
                else:
                    inv_neu = 1.0 / common
                for j, face in enumerate(faces):
                    (co_n if own else co_o)[j, plane, here, :] = face * inv_neu
                (inv_n if own else inv_o)[plane, here, :] = inv_neu

    coefficients(lab, buf_a, exists, True)

    pl.when(stays)(keep[2].wait)
    pl.when(swapped)(swap_u.wait_recv)

    last = TICKS - 1

    def inner_jump(t, n, carry):
        got_q(1 - core, t, n).wait_recv()
        for row in range(0, NY, CHUNK):
            here = slice(row, row + CHUNK)
            jump_in[t, n, here, :] = qs[1 - core, t, n, here, :] + qr[1 - core, t, n, here, :]
        if t < last:
            send_jump(t, n).start()
        else:
            pl.when(outer_left)(send_jump(t, n).start)
        return carry

    def outer(t, n):
        send_jump(t, n).wait_recv()
        near, far = 1 - core, core
        for row in range(0, NY, CHUNK):
            here = slice(row, row + CHUNK)
            rows = slice(PAD + row, PAD + row + CHUNK)
            jump = qs[core, t, n, here, :] + qr[core, t, n, here, :]
            rhs[near, here, :] = inv_o[near, here, :] * jump + co_o[5, near, here, :] * psi_o[near, rows, :]
            rhs[far, here, :] = (
                inv_o[far, here, :] * jump_far[t, n, here, :] + co_o[5, far, here, :] * psi_o[far, rows, :]
            )
        sweep(psi_o, buf_a, rhs, co_o)
        sweep(buf_a, buf_b, rhs, co_o)
        sweep(buf_b, psi_o, rhs, co_o)
        for row in range(0, NY, CHUNK):
            pr[core, t, n, row : row + CHUNK, :] = psi_o[near, PAD + row : PAD + row + CHUNK, :]

    def finish(n, carry, solve=True):
        if solve:
            pl.when(outer_right)(lambda: outer(last, n))
        pl.when(p_uses[1])(got_p(1, last, n).wait_recv)
        for row in range(0, NY, CHUNK):
            here = slice(row, row + CHUNK)
            new = h_right[n, here, :] + 0.25 * (ps[1, last, n, here, :] + pr[1, last, n, here, :])
            back[n, here, :] = jnp.where(has_right, new, 0.0)
        send_home(n).start()
        return carry

    for tick in range(TICKS):
        state = u.at[tick]
        if tick > 0:
            pl.when(jnp.logical_and(restart[tick], has_left))(pass_guess.wait_recv)

        def dirichlet(n, carry, tick=tick, state=state):
            if tick == 0:
                pl.when(has_left)(pass_h(n).wait_recv)
            else:
                if tick == 1:
                    pl.when(has_right)(pass_h(n).wait_send)

                @pl.when(useful[tick - 1])
                def _():
                    pl.when(long)(lambda: outer(tick - 1, n))
                    for side, trace in enumerate((h_left, h_right)):
                        pl.when(p_uses[side])(got_p(side, tick - 1, n).wait_recv)
                        for row in range(0, NY, CHUNK):
                            here = slice(row, row + CHUNK)
                            both = ps[side, tick - 1, n, here, :] + pr[side, tick - 1, n, here, :]
                            new = trace[n, here, :] + 0.25 * both
                            trace[n, here, :] = jnp.where(exists[side], new, 0.0)

                @pl.when(restart[tick])
                def _():
                    for side, (trace, taken) in enumerate(((h_left, guess_left), (h_right, guess_right))):
                        for row in range(0, NY, CHUNK):
                            here = slice(row, row + CHUNK)
                            trace[n, here, :] = jnp.where(exists[side], taken[n, here, :], 0.0)

                pl.when(n == 0)(move_u[tick - 1].wait_recv)

            for plane, trace in enumerate((h_left, h_right)):
                for row in range(0, NY, CHUNK):
                    here = slice(row, row + CHUNK)
                    rhs[plane, here, :] = (
                        co_d[5, plane, here, :] * state[plane, PAD + row : PAD + row + CHUNK, :]
                        + co_d[6, plane, here, :] * trace[n, here, :]
                    )

            def flux(plane, here, value):
                trace = (h_left, h_right)[plane]
                qs[plane, tick, n, here, :] = end[plane, here, :] * (value - trace[n, here, :])

            sweep(state, buf_a, rhs, co_d)
            sweep(buf_a, buf_b, rhs, co_d)
            sweep(buf_b, state, rhs, co_d, flux)
            pl.when(jnp.logical_and(has_right, useful[tick]))(send_q(1, tick, n).start)
            pl.when(jnp.logical_and(has_left, useful[tick]))(send_q(0, tick, n).start)
            return carry

        lax.fori_loop(0, STEPS, dirichlet, 0)
        if tick + 1 < TICKS:
            move_u[tick].start()
        else:
            home_u.start()
        if tick + 1 < TICKS:

            @pl.when(jnp.logical_and(swapped, restart[tick + 1]))
            def _():
                swap_guess.wait_recv()
                pl.when(has_right)(pass_guess.start)

        @pl.when(jnp.logical_and(long, useful[tick]))
        def _():
            lax.fori_loop(0, STEPS, functools.partial(inner_jump, tick), 0)

        def neumann(n, carry, tick=tick, first=False):
            for side in range(2):
                pl.when(q_wait[side])(got_q(side, tick, n).wait_recv)
            for plane in range(2):
                for row in range(0, NY, CHUNK):
                    here = slice(row, row + CHUNK)
                    jump = qs[plane, tick, n, here, :] + qr[plane, tick, n, here, :]
                    value = inv_n[plane, here, :] * jnp.where(exists[plane], jump, 0.0)
                    if not first:
                        value = value + co_n[5, plane, here, :] * psi[plane, PAD + row : PAD + row + CHUNK, :]
                    rhs[plane, here, :] = value
                    if first:
                        buf_a[plane, PAD + row : PAD + row + CHUNK, :] = value

            def ends(plane, here, value):
                ps[plane, tick, n, here, :] = value

            if not first:
                sweep(psi, buf_a, rhs, co_n)
            sweep(buf_a, buf_b, rhs, co_n)
            sweep(buf_b, psi, rhs, co_n, ends)
            pl.when(p_uses[0])(send_p(0, tick, n).start)
            if tick + 1 < TICKS:
                pl.when(p_uses[1])(send_p(1, tick, n).start)
            else:
                @pl.when(outer_left)
                def _():
                    finish(n, 0, False)

                if not first:

                    @pl.when(lagging)
                    def _():
                        finish(n - 1, 0, False)

            return carry

        @pl.when(useful[tick])
        def _():
            neumann(0, 0, first=True)

        @pl.when(long)
        def _():
            if tick == 0:
                send_lab.wait_recv()
                coefficients(lab_o, psi_o, None, False)
            psi_o[:, PAD : PAD + NY, :] = jnp.zeros((2, NY, NZ), F32)

        @pl.when(useful[tick])
        def _():
            lax.fori_loop(1, STEPS, neumann, 0)


    @pl.when(core == 1)
    def _():
        lax.fori_loop(0, STEPS, finish, 0)

    @pl.when(lagging)
    def _():
        finish(STEPS - 1, 0, False)


    @pl.when(swapped)
    def _():
        for copy in swap_h:
            copy.wait_send()
        swap_lab.wait_send()
        swap_u.wait_send()

    pl.when(jnp.logical_and(swapped, takes_guess))(swap_guess.wait_send)
    pl.when(jnp.logical_and(takes_guess, has_right))(pass_guess.wait_send)
    for copy in move_u:
        copy.wait_send()
    home_u.wait_send()

    for side in range(2):

        @pl.when(exists[side])
        def _():
            for n in range(STEPS):
                for t in range(TICKS):
                    pl.when(useful[t])(send_q(side, t, n).wait_send)

        @pl.when(p_uses[side])
        def _():
            for n in range(STEPS):
                for t in range(TICKS if side == 0 else last):
                    pl.when(useful[t])(send_p(side, t, n).wait_send)

    @pl.when(long)
    def _():
        send_lab.wait_send()
        for n in range(STEPS):
            for t in range(last):
                pl.when(useful[t])(send_jump(t, n).wait_send)

    @pl.when(outer_left)
    def _():
        for n in range(STEPS):
            send_jump(last, n).wait_send()

    for n in range(STEPS):
        send_home(n).wait_send()
    home_u.wait_recv()
    for n in range(STEPS):
        send_home(n).wait_recv()


def deliver(field, trace, out_field, out_trace, block, in_sem, out_sem):
    pieces = [(field.at[0, i], out_field.at[0, i]) for i in range(2)]
    pieces += [(trace.at[0, 0, n], out_trace.at[0, 0, n]) for n in range(STEPS)]
    loads = [pltpu.make_async_copy(src, block.at[i], in_sem.at[i]) for i, (src, _) in enumerate(pieces)]
    stores = [pltpu.make_async_copy(block.at[i], dst, out_sem.at[i]) for i, (_, dst) in enumerate(pieces)]
    for copy in loads:
        copy.start()
    for load, store in zip(loads, stores):
        load.wait()
        store.start()
    for store in stores:
        store.wait()


def local(fields, labels, traces, new_guess, cond_table, cap_table):
    plane = (NY, NZ)
    field = (2, ROWS, NZ)
    vm = lambda *shape: pltpu.VMEM(shape, F32)
    dma = lambda *shape: pltpu.SemaphoreType.DMA(shape)
    any_spec = pl.BlockSpec(memory_space=pl.ANY)
    hbm = pl.BlockSpec(memory_space=pltpu.HBM)
    per_step = (TICKS, STEPS) + plane
    results = pl.pallas_call(
        kernel,
        out_shape=(
            jax.ShapeDtypeStruct((1, 2) + plane, F32),
            jax.ShapeDtypeStruct((1, 1, STEPS) + plane, F32),
        ),
        in_specs=[hbm] * 6,
        out_specs=(any_spec, any_spec),
        scratch_shapes=[
            pltpu.SMEM((4,), F32),
            pltpu.SMEM((4,), F32),
            pltpu.VMEM((2,) + plane, jnp.int32),
            vm(2, *plane),
            vm(STEPS, *plane),
            pltpu.VMEM((2,) + plane, jnp.int32),
            vm(TICKS, *field),
            vm(STEPS, *plane),
            vm(STEPS, *plane),
            vm(STEPS, *plane),
            vm(STEPS, *plane),
            vm(*field),
            vm(*field),
            vm(*field),
            vm(2, *plane),
            vm(7, 2, *plane),
            vm(6, 2, *plane),
            vm(2, *plane),
            vm(2, *plane),
            vm(2, *per_step),
            vm(2, *per_step),
            vm(2, *per_step),
            vm(2, *per_step),
            vm(STEPS, *plane),
            pltpu.VMEM((2,) + plane, jnp.int32),
            vm(6, 2, *plane),
            vm(2, *plane),
            vm(*field),
            vm(*per_step),
            vm(*per_step),
            pltpu.SemaphoreType.DMA,
            dma(TICKS),
            dma(STEPS),
            dma(STEPS),
            pltpu.SemaphoreType.DMA,
            pltpu.SemaphoreType.DMA,
            dma(TICKS, 2, STEPS),
            dma(TICKS, 2, STEPS),
            dma(STEPS + 1),
            dma(6),
            dma(8 + TICKS + 2),
            dma(TICKS, 2, STEPS),
            dma(TICKS, 2, STEPS),
            dma(STEPS),
            dma(STEPS),
            pltpu.SemaphoreType.DMA,
            dma(TICKS, STEPS),
            dma(TICKS, STEPS),
        ],
        compiler_params=pltpu.CompilerParams(collective_id=0, has_side_effects=True),
    )(cond_table, cap_table, fields, labels, traces, new_guess)
    return pl.pallas_call(
        deliver,
        out_shape=(
            jax.ShapeDtypeStruct((1, 2) + plane, F32),
            jax.ShapeDtypeStruct((1, 1, STEPS) + plane, F32),
        ),
        in_specs=[any_spec] * 2,
        out_specs=(any_spec, any_spec),
        scratch_shapes=[vm(2 + STEPS, *plane), dma(2 + STEPS), dma(2 + STEPS)],
    )(*results)


def solution(mesh):
    return jax.shard_map(
        local,
        mesh=mesh,
        in_specs=(
            P("iter", "sub", None, None),
            P("sub", None, None),
            P("iter", "sub", None, None, None),
            P(None, "sub", None, None, None),
            P(),
            P(),
        ),
        out_specs=(P("iter", "sub", None, None), P("iter", "sub", None, None, None)),
        check_vma=False,
    )
```
